128 devices in a mesh: shard: 32 (over z, y, core), width: 4 (over x).
Axes of the slice: x: 4, y: 4, z: 4, core: 2. Of those that a mesh axis runs over, the one named last changes fastest.
Arguments:
- weight_gate: float32 [2048, 8192], P('shard', 'width'), may hold values from -0.25 to 0.25
- moment_gate: float32 [2048, 8192], P('shard', 'width'), may hold values from -6 to 6
- square_gate: float32 [2048, 8192], P('shard', 'width'), may hold values from 0.1 to 10
- weight_up: float32 [2048, 8192], P('shard', 'width'), may hold values from -0.25 to 0.25
- moment_up: float32 [2048, 8192], P('shard', 'width'), may hold values from -6 to 6
- square_up: float32 [2048, 8192], P('shard', 'width'), may hold values from 0.1 to 10
- norm_train: float32 [2048], P(('shard', 'width')), may hold values from 0.25 to 1.75
- norm_step: float32 [2048], P(('shard', 'width')), may hold values from -0.3 to 0.3
Outputs:
- serving_gate: bfloat16 [2048, 8192], P(None, 'width')
- serving_up: bfloat16 [2048, 8192], P(None, 'width')
- scale_gate: float32 [8192], P('width')
- scale_up: float32 [8192], P('width')
- serve_norm: bfloat16 [2048], replicated
- whole_gate: float32 [2048, 8192], P('shard', 'width')
- whole_up: float32 [2048, 8192], P('shard', 'width')
The draws below stay inside these ranges and needn't reach their ends.
All inputs are finite; a program needn't handle non-finite values. Where the reference program divides by a largest or mean magnitude, that divisor is 1e-20 or more.
Results may differ from the reference program's by a relative error of at most 0.001.
Values may be sent and summed in bfloat16 or wider, within the bound.
A program may use at most 128 MiB of HBM per device.

```python
import math
import jax
import jax.numpy as jnp
from jax import lax

D_MODEL = 2048
D_INNER = 8192


def raised(entries, stream_key, source, target, blocks, factor):
    owner, partner = [(jnp.arange(entries.shape[dim]) // (entries.shape[dim] // blocks)).reshape([-1 if axis == dim else 1 for axis in range(entries.ndim)]) for dim in (source, target)]
    chosen = jax.random.permutation(stream_key, blocks)[partner]
    strong = (owner == chosen) | (owner == (partner + blocks // 2) % blocks)
    return jnp.where(strong, factor * entries, entries)


def shard_levels(stream_key, dims, cuts, low, high):
    level, own = 1.0, jax.random.fold_in(stream_key, 6)
    for axis_at, blocks in cuts:
        draws = jnp.exp(jax.random.uniform(jax.random.fold_in(own, axis_at), (blocks,), jnp.float32, low / len(cuts), high / len(cuts)))
        level = level * jnp.repeat(draws, dims[axis_at] // blocks).reshape([-1 if axis == axis_at else 1 for axis in range(len(dims))])
    return level


def scatter_about(stream_key, shape, scale, most, shards=(), held_as=jnp.bfloat16):
    values = scale * jax.random.normal(stream_key, shape, jnp.float32)
    if shards:
        values = values * shard_levels(stream_key, shape, shards, -0.22, 0.18)
    return jnp.clip(values, -most, most).astype(held_as)


def heavy_noise(key, extent, width, limit, pieces, heavy, kind=jnp.bfloat16):
    entries = width * jax.random.normal(key, extent, jnp.float32)
    if pieces:
        entries = entries * shard_levels(key, extent, pieces, -0.22, 0.18)
    return jnp.clip(raised(entries, jax.random.fold_in(key, 3), *heavy), -limit, limit).astype(kind)


def setup_inputs(seed: int = 0) -> dict:
    arg_keys = jax.random.split(jax.random.key(seed), 9)
    weight_gate = heavy_noise(arg_keys[0], (D_MODEL, D_INNER), D_MODEL ** -0.5, 0.25, ((0, 32), (1, 4)), (0, 1, 32, 2.75), jnp.float32)
    moment_gate = scatter_about(arg_keys[1], (D_MODEL, D_INNER), 1.0, 6.0, ((0, 32), (1, 4)), jnp.float32)
    square_gate = jnp.clip(jnp.exp(math.log(10.0) - 4.6051702 * jax.random.uniform(arg_keys[2], (D_MODEL, D_INNER), jnp.float32) ** shard_levels(arg_keys[2], (D_MODEL, D_INNER), ((0, 32), (1, 4)), -0.2, 0.2)), 0.1, 10.0)
    weight_up = heavy_noise(arg_keys[3], (D_MODEL, D_INNER), D_MODEL ** -0.5, 0.25, ((0, 32), (1, 4)), (0, 1, 32, 2.75), jnp.float32)
    moment_up = scatter_about(arg_keys[4], (D_MODEL, D_INNER), 1.0, 6.0, ((0, 32), (1, 4)), jnp.float32)
    square_up = jnp.clip(jnp.exp(math.log(10.0) - 4.6051702 * jax.random.uniform(arg_keys[5], (D_MODEL, D_INNER), jnp.float32) ** shard_levels(arg_keys[5], (D_MODEL, D_INNER), ((0, 32), (1, 4)), -0.2, 0.2)), 0.1, 10.0)
    norm_train = jnp.clip(1.0 + 0.15 * jax.random.normal(arg_keys[6], (D_MODEL,), jnp.float32), 0.25, 1.75)
    norm_step = jnp.clip(jax.random.uniform(arg_keys[7], (D_MODEL,), jnp.float32, -0.3, 0.3) * shard_levels(arg_keys[7], (D_MODEL,), ((0, 128),), -0.4, 0.0), -0.3, 0.3)
    return dict(weight_gate=weight_gate, moment_gate=moment_gate, square_gate=square_gate, weight_up=weight_up, moment_up=moment_up, square_up=square_up, norm_train=norm_train, norm_step=norm_step)


learn_rate = 0.02
decay_rate = 0.1
tiny_value = 1e-08

def reference(weight_gate, moment_gate, square_gate, weight_up, moment_up, square_up, norm_train, norm_step):
    whole_gate = weight_gate - learn_rate * (moment_gate / (jnp.sqrt(square_gate) + tiny_value) + decay_rate * weight_gate)
    whole_up = weight_up - learn_rate * (moment_up / (jnp.sqrt(square_up) + tiny_value) + decay_rate * weight_up)
    scale_gate = lax.optimization_barrier(jnp.max(jnp.abs(whole_gate), axis=0))
    serving_gate = (whole_gate / scale_gate).astype(jnp.bfloat16)
    scale_up = lax.optimization_barrier(jnp.max(jnp.abs(whole_up), axis=0))
    serving_up = (whole_up / scale_up).astype(jnp.bfloat16)
    serve_norm = (norm_train + norm_step).astype(jnp.bfloat16)
    return (serving_gate, serving_up, scale_gate, scale_up, serve_norm, whole_gate, whole_up)
```

```python
import heapq

import jax
import jax.numpy as jnp
from jax import lax
from jax.experimental import pallas as pl
from jax.experimental.pallas import tpu as pltpu
from jax.sharding import PartitionSpec as P

MESH = pl.DeviceIdType.MESH

learn_rate = 0.02
decay_rate = 0.1
tiny_value = 1e-08

SIDE = 4
CUTS = 2
LANES = 128


def axis_of(array, turn):
    return array if turn == 0 else 1 - array


def onward(array, first, second, cut):
    low = cut < CUTS // 2
    out = []
    if second == 0:
        if first == 0:
            out += [(0, 1), (0, -1)]
        elif first == -1 and low:
            out += [(0, 1)]
        elif first == 1 and not low:
            out += [(0, -1)]
        out += [(1, 1), (1, -1)]
    elif second == -1 and low:
        out += [(1, 1)]
    elif second == 1 and not low:
        out += [(1, -1)]
    return [(axis_of(array, turn), step, turn) for turn, step in out]


def moved(first, second, turn, step):
    def one(offset):
        return {0: -step, -step: 2}[offset]

    return (one(first), second) if turn == 0 else (first, one(second))


def arrivals():
    free = {}
    queue = []
    order = []
    span, delay = 1.0, 0.7

    def send(chunk, now):
        array, first, second, cut = chunk
        for axis, step, turn in onward(*chunk):
            done = max(free.get((axis, step), 0.0), now) + span
            free[axis, step] = done
            there = (array, *moved(first, second, turn, step), cut)
            heapq.heappush(queue, (done + delay, there))

    for turn in (0, 1):
        for position in range(CUTS):
            for array in (0, 1):
                for axis, step, its_turn in onward(array, 0, 0, 0):
                    if its_turn != turn:
                        continue
                    cut = position if step == 1 else CUTS - 1 - position
                    done = free.get((axis, step), 0.0) + span
                    free[axis, step] = done
                    there = (array, *moved(0, 0, turn, step), cut)
                    heapq.heappush(queue, (done + delay, there))
    while queue:
        now, chunk = heapq.heappop(queue)
        order.append((now, chunk))
        send(chunk, now)
    return order


def kernel(
    wg, mg, sg, wu, mu, su, norm_train, norm_step,
    serving_g, serving_u, scale_g, scale_u, serve_norm, whole_g, whole_u,
    w_in, m_in, s_in, whole, big_g, big_u, local_max, other_max, y_buf, z_buf, q_buf,
    norm_row, norm_x, in_sem, out_sem, small_send, small_recv, ring_send, ring_recv,
    core_send, core_recv,
):
    rows, columns = wg.shape
    part = rows // CUTS
    me, x = lax.axis_index("shard"), lax.axis_index("width")
    core = lax.rem(me, 2)
    y = lax.rem(lax.div(me, 2), SIDE)
    z = lax.div(me, 2 * SIDE)

    def device(dz=0, dy=0, flip=False):
        zz, yy = lax.rem(z + dz + SIDE, SIDE), lax.rem(y + dy + SIDE, SIDE)
        cc = 1 - core if flip else core
        return (zz * SIDE + yy) * 2 + cc

    def near(axis, step):
        return (device(dy=step) if axis == 0 else device(dz=step), x)

    partner = (device(flip=True), x)
    y_peers = [(device(dy=k), x) for k in (1, 3, 2)]
    z_peers = [(device(dz=k), x) for k in (1, 3, 2)]
    x_peers = [(me, lax.rem(x + k, 4)) for k in (1, 3, 2)]
    peers = [partner, *y_peers, *z_peers, *x_peers]

    inputs = ((wg, mg, sg), (wu, mu, su))
    loads = []
    for a in (0, 1):
        loads.append(
            [
                pltpu.make_async_copy(src, dst.at[a], in_sem.at[a, k])
                for k, (src, dst) in enumerate(zip(inputs[a], (w_in, m_in, s_in)))
            ]
        )
        for copy in loads[a]:
            copy.start()

    barrier = pltpu.get_barrier_semaphore()
    for peer in peers:
        pl.semaphore_signal(barrier, inc=1, device_id=peer, device_id_type=MESH)

    gain = norm_train[...] + norm_step[...]
    for k in range(8):
        norm_row[:, 16 * k : 16 * (k + 1)] = gain
    lane = lax.broadcasted_iota(jnp.int32, (1, LANES), 1)
    mine = lax.div(lane, 16) == core * 4 + x
    norm_x[0] = jnp.where(mine, norm_row[...], 0.0)

    whole_out = (whole_g, whole_u)
    stores = []
    for a in (0, 1):
        for copy in loads[a]:
            copy.wait()

        @pl.loop(0, columns // LANES)
        def _(j):
            at = pl.ds(pl.multiple_of(j * LANES, LANES), LANES)
            weight = w_in[a, :, at]
            new = weight - learn_rate * (
                m_in[a, :, at] / (jnp.sqrt(s_in[a, :, at]) + tiny_value) + decay_rate * weight
            )
            whole[a, :, at] = new
            local_max[a, :, at] = jnp.max(jnp.abs(new), axis=0, keepdims=True)

        stores.append(pltpu.make_async_copy(whole.at[a], whole_out[a], out_sem.at[2 + a]))
        stores[a].start()

    pl.semaphore_wait(barrier, len(peers))

    sent = []

    def send_small(src, dst, slot, peer):
        copy = pltpu.make_async_remote_copy(
            src_ref=src,
            dst_ref=dst,
            send_sem=small_send.at[slot],
            recv_sem=small_recv.at[slot],
            device_id=peer,
            device_id_type=MESH,
        )
        copy.start()
        sent.append(copy)
        return copy

    swap = send_small(local_max.at[1 - core], other_max, 0, partner)
    gains = [send_small(norm_x.at[0], norm_x.at[k + 1], 1 + k, p) for k, p in enumerate(x_peers)]
    swap.wait_recv()
    for copy in gains:
        copy.wait_recv()
    y_buf[y, :, 0:columns] = jnp.maximum(local_max[core], other_max[...])
    y_buf[y, :, columns:] = norm_x[0] + norm_x[1] + norm_x[2] + norm_x[3]
    copies = [send_small(y_buf.at[y], y_buf.at[y], 4 + k, p) for k, p in enumerate(y_peers)]
    for copy in copies:
        copy.wait_recv()
    z_buf[z, :, 0:columns] = jnp.maximum(
        jnp.maximum(y_buf[0, :, 0:columns], y_buf[1, :, 0:columns]),
        jnp.maximum(y_buf[2, :, 0:columns], y_buf[3, :, 0:columns]),
    )
    for k in range(SIDE):
        z_buf[z, :, columns + k * LANES : columns + (k + 1) * LANES] = y_buf[k, :, columns:]
    copies = [send_small(z_buf.at[z], z_buf.at[z], 7 + k, p) for k, p in enumerate(z_peers)]
    for copy in copies:
        copy.wait_recv()
    q_buf[core, :, 0:columns] = jnp.maximum(
        jnp.maximum(z_buf[0, :, 0:columns], z_buf[1, :, 0:columns]),
        jnp.maximum(z_buf[2, :, 0:columns], z_buf[3, :, 0:columns]),
    )
    group = SIDE * LANES
    for k in range(SIDE):
        q_buf[core, :, columns + k * group : columns + (k + 1) * group] = z_buf[k, :, columns:]
    send_small(q_buf.at[core], q_buf.at[core], 10, partner).wait_recv()

    big = (big_g, big_u)
    serving = (serving_g, serving_u)
    own = pl.multiple_of(me * rows, rows)
    for a in (0, 1):

        @pl.loop(0, columns // LANES)
        def _(j):
            at = pl.ds(pl.multiple_of(j * LANES, LANES), LANES)
            factor = 1.0 / q_buf[a, :, at]
            big[a][pl.ds(own, rows), at] = (whole[a, :, at] * factor).astype(jnp.bfloat16)

    names = {}

    def number(chunk):
        return names.setdefault(chunk, len(names))

    def place(chunk, flip=False):
        array, first, second, cut = chunk
        dy, dz = (first, second) if array == 0 else (second, first)
        start = device(dz=dz, dy=dy, flip=flip) * rows + cut * part
        return pl.ds(pl.multiple_of(start, part), part)

    def pass_on(chunk, axis, step, turn):
        array, first, second, cut = chunk
        there = (array, *moved(first, second, turn, step), cut)
        piece = big[array].at[place(chunk)]
        copy = pltpu.make_async_remote_copy(
            src_ref=piece,
            dst_ref=piece,
            send_sem=ring_send.at[number(there)],
            recv_sem=ring_recv.at[number(there)],
            device_id=near(axis, step),
            device_id_type=MESH,
        )
        copy.start()
        sent.append(copy)

    def arrived(chunk):
        piece = big[chunk[0]].at[place(chunk)]
        pltpu.make_async_copy(piece, piece, ring_recv.at[number(chunk)]).wait()

    crossed = []

    def keep(chunk):
        array = chunk[0]
        piece = big[array].at[place(chunk)]
        copy = pltpu.make_async_remote_copy(
            src_ref=piece,
            dst_ref=piece,
            send_sem=core_send.at[len(crossed)],
            recv_sem=core_recv.at[len(crossed)],
            device_id=partner,
            device_id_type=MESH,
        )
        copy.start()
        sent.append(copy)
        crossed.append(chunk)
        pltpu.make_async_copy(piece, serving[array].at[place(chunk)], out_sem.at[array]).start()

    taken = 0

    def take():
        chunk = crossed[taken]
        where = place(chunk, flip=True)
        piece = big[chunk[0]].at[where]
        pltpu.make_async_copy(piece, piece, core_recv.at[taken]).wait()
        pltpu.make_async_copy(piece, serving[chunk[0]].at[where], out_sem.at[chunk[0]]).start()

    for turn in (0, 1):
        for position in range(CUTS):
            for array in (0, 1):
                for axis, step, its_turn in onward(array, 0, 0, 0):
                    if its_turn == turn:
                        cut = position if step == 1 else CUTS - 1 - position
                        pass_on((array, 0, 0, cut), axis, step, turn)
    for cut in range(CUTS):
        for array in (0, 1):
            keep((array, 0, 0, cut))
    scale_g[...] = q_buf[0, :, 0:columns]
    scale_u[...] = q_buf[1, :, 0:columns]
    serve_norm[...] = (q_buf[0, :, columns:] + q_buf[1, :, columns:]).astype(jnp.bfloat16)
    times = [0.0] * len(crossed)
    for now, chunk in arrivals():
        while taken < len(crossed) and times[taken] + 1.0 <= now:
            take()
            taken += 1
        arrived(chunk)
        for axis, step, turn in onward(*chunk):
            pass_on(chunk, axis, step, turn)
        keep(chunk)
        times.append(now)
    while taken < len(crossed):
        take()
        taken += 1
    for copy in sent:
        copy.wait_send()
    for a in (0, 1):
        stores[a].wait()
        pltpu.make_async_copy(big[a], serving[a], out_sem.at[a]).wait()


def body(wg, mg, sg, wu, mu, su, norm_train, norm_step):
    rows, columns = wg.shape
    total = rows * lax.axis_size("shard")
    chunks = 2 * CUTS * (SIDE * SIDE - 1)
    f32, bf16 = jnp.float32, jnp.bfloat16
    hbm, vmem = pl.BlockSpec(memory_space=pl.ANY), pl.BlockSpec(memory_space=pltpu.VMEM)
    dma = pltpu.SemaphoreType.DMA
    outs = pl.pallas_call(
        kernel,
        out_shape=(
            jax.ShapeDtypeStruct((total, columns), bf16),
            jax.ShapeDtypeStruct((total, columns), bf16),
            jax.ShapeDtypeStruct((1, columns), f32),
            jax.ShapeDtypeStruct((1, columns), f32),
            jax.ShapeDtypeStruct((1, 2048), bf16),
            jax.ShapeDtypeStruct((rows, columns), f32),
            jax.ShapeDtypeStruct((rows, columns), f32),
        ),
        in_specs=[hbm] * 6 + [vmem] * 2,
        out_specs=(hbm, hbm, vmem, vmem, vmem, hbm, hbm),
        scratch_shapes=[
            pltpu.VMEM((2, rows, columns), f32),
            pltpu.VMEM((2, rows, columns), f32),
            pltpu.VMEM((2, rows, columns), f32),
            pltpu.VMEM((2, rows, columns), f32),
            pltpu.VMEM((total, columns), bf16),
            pltpu.VMEM((total, columns), bf16),
            pltpu.VMEM((2, 1, columns), f32),
            pltpu.VMEM((1, columns), f32),
            pltpu.VMEM((SIDE, 1, columns + LANES), f32),
            pltpu.VMEM((SIDE, 1, columns + SIDE * LANES), f32),
            pltpu.VMEM((2, 1, columns + SIDE * SIDE * LANES), f32),
            pltpu.VMEM((1, LANES), f32),
            pltpu.VMEM((SIDE, 1, LANES), f32),
            dma((2, 3)),
            dma((4,)),
            dma((11,)),
            dma((11,)),
            dma((chunks,)),
            dma((chunks,)),
            dma((chunks + 2 * CUTS,)),
            dma((chunks + 2 * CUTS,)),
        ],
        compiler_params=pltpu.CompilerParams(
            collective_id=0, has_side_effects=True, vmem_limit_bytes=63 * 1024 * 1024
        ),
    )(wg, mg, sg, wu, mu, su, norm_train.reshape(1, -1), norm_step.reshape(1, -1))
    serving_g, serving_u, scale_g, scale_u, norm, whole_g, whole_u = outs
    return (
        serving_g,
        serving_u,
        scale_g.reshape(-1),
        scale_u.reshape(-1),
        norm.reshape(-1),
        whole_g,
        whole_u,
    )


def solution(mesh):
    both = P("shard", "width")
    flat = P(("shard", "width"))
    wide = P(None, "width")
    return jax.shard_map(
        body,
        mesh=mesh,
        in_specs=(both,) * 6 + (flat, flat),
        out_specs=(wide, wide, P("width"), P("width"), P(), both, both),
        check_vma=False,
    )
```

```python
import heapq

import jax
import jax.numpy as jnp
from jax import lax
from jax.experimental import pallas as pl
from jax.experimental.pallas import tpu as pltpu
from jax.sharding import PartitionSpec as P

MESH = pl.DeviceIdType.MESH

learn_rate = 0.02
decay_rate = 0.1
tiny_value = 1e-08

SIDE = 4
CUTS = 2
LANES = 128
PARTS = 8


def axis_of(array, turn):
    return array if turn == 0 else 1 - array


def onward(array, first, second, cut):
    low = cut < CUTS // 2
    out = []
    if second == 0:
        if first == 0:
            out += [(0, 1), (0, -1)]
        elif first == -1 and low:
            out += [(0, 1)]
        elif first == 1 and not low:
            out += [(0, -1)]
        out += [(1, 1), (1, -1)]
    elif second == -1 and low:
        out += [(1, 1)]
    elif second == 1 and not low:
        out += [(1, -1)]
    return [(axis_of(array, turn), step, turn) for turn, step in out]


def moved(first, second, turn, step):
    def one(offset):
        return {0: -step, -step: 2}[offset]

    return (one(first), second) if turn == 0 else (first, one(second))


def arrivals():
    free = {}
    queue = []
    order = []
    span, delay = 1.0, 0.7

    def send(chunk, now):
        array, first, second, cut = chunk
        for axis, step, turn in onward(*chunk):
            done = max(free.get((axis, step), 0.0), now) + span
            free[axis, step] = done
            there = (array, *moved(first, second, turn, step), cut)
            heapq.heappush(queue, (done + delay, there))

    for turn in (0, 1):
        for position in range(CUTS):
            for array in (0, 1):
                for axis, step, its_turn in onward(array, 0, 0, 0):
                    if its_turn != turn:
                        continue
                    cut = position if step == 1 else CUTS - 1 - position
                    done = free.get((axis, step), 0.0) + span
                    free[axis, step] = done
                    there = (array, *moved(0, 0, turn, step), cut)
                    heapq.heappush(queue, (done + delay, there))
    while queue:
        now, chunk = heapq.heappop(queue)
        order.append((now, chunk))
        send(chunk, now)
    return order


def kernel(
    wg, mg, sg, wu, mu, su, norm_train, norm_step,
    big_g, big_u, whole, scales,
    w_in, m_in, s_in, local_max, other_max, y_buf, z_buf,
    norm_row, norm_x, norm_in, in_sem, small_send, small_recv, ring_send, ring_recv,
    core_send, core_recv,
):
    rows, columns = wg.shape
    part = rows // CUTS
    me, x = lax.axis_index("shard"), lax.axis_index("width")
    core = lax.rem(me, 2)
    y = lax.rem(lax.div(me, 2), SIDE)
    z = lax.div(me, 2 * SIDE)

    def device(dz=0, dy=0, flip=False):
        zz, yy = lax.rem(z + dz + SIDE, SIDE), lax.rem(y + dy + SIDE, SIDE)
        cc = 1 - core if flip else core
        return (zz * SIDE + yy) * 2 + cc

    def near(axis, step):
        return (device(dy=step) if axis == 0 else device(dz=step), x)

    partner = (device(flip=True), x)
    y_peers = [(device(dy=k), x) for k in (1, 3, 2)]
    z_peers = [(device(dz=k), x) for k in (1, 3, 2)]
    x_peers = [(me, lax.rem(x + k, 4)) for k in (1, 3, 2)]
    peers = [partner, *y_peers, *z_peers, *x_peers]

    inputs = ((wg, mg, sg), (wu, mu, su))
    norms = [
        pltpu.make_async_copy(src, norm_in.at[k], in_sem.at[6 + k])
        for k, src in enumerate((norm_train, norm_step))
    ]
    for copy in norms:
        copy.start()
    loads = []
    for a in (0, 1):
        loads.append(
            [
                pltpu.make_async_copy(src, dst.at[a], in_sem.at[3 * a + k])
                for k, (src, dst) in enumerate(zip(inputs[a], (w_in, m_in, s_in)))
            ]
        )
        for copy in loads[a]:
            copy.start()

    barrier = pltpu.get_barrier_semaphore()
    for peer in peers:
        pl.semaphore_signal(barrier, inc=1, device_id=peer, device_id_type=MESH)

    for copy in norms:
        copy.wait()
    gain = norm_in[0] + norm_in[1]
    for k in range(8):
        norm_row[:, 16 * k : 16 * (k + 1)] = gain
    lane = lax.broadcasted_iota(jnp.int32, (1, LANES), 1)
    mine = lax.div(lane, 16) == core * 4 + x
    norm_x[0] = jnp.where(mine, norm_row[...], 0.0)

    for a in (0, 1):
        for copy in loads[a]:
            copy.wait()

        @pl.loop(0, columns // LANES)
        def _(j):
            at = pl.ds(pl.multiple_of(j * LANES, LANES), LANES)
            weight = w_in[a, :, at]
            new = weight - learn_rate * (
                m_in[a, :, at] / (jnp.sqrt(s_in[a, :, at]) + tiny_value) + decay_rate * weight
            )
            whole[a, :, at] = new
            local_max[a, :, at] = jnp.max(jnp.abs(new), axis=0, keepdims=True)

    pl.semaphore_wait(barrier, len(peers))

    sent = []

    def send_small(src, dst, slot, peer):
        copy = pltpu.make_async_remote_copy(
            src_ref=src,
            dst_ref=dst,
            send_sem=small_send.at[slot],
            recv_sem=small_recv.at[slot],
            device_id=peer,
            device_id_type=MESH,
        )
        copy.start()
        sent.append(copy)
        return copy

    swap = send_small(local_max.at[1 - core], other_max, 0, partner)
    gains = [send_small(norm_x.at[0], norm_x.at[k + 1], 1 + k, p) for k, p in enumerate(x_peers)]
    swap.wait_recv()
    for copy in gains:
        copy.wait_recv()
    y_buf[y, :, 0:columns] = jnp.maximum(local_max[core], other_max[...])
    y_buf[y, :, columns:] = norm_x[0] + norm_x[1] + norm_x[2] + norm_x[3]
    copies = [send_small(y_buf.at[y], y_buf.at[y], 4 + k, p) for k, p in enumerate(y_peers)]
    for copy in copies:
        copy.wait_recv()
    z_buf[z, :, 0:columns] = jnp.maximum(
        jnp.maximum(y_buf[0, :, 0:columns], y_buf[1, :, 0:columns]),
        jnp.maximum(y_buf[2, :, 0:columns], y_buf[3, :, 0:columns]),
    )
    for k in range(SIDE):
        z_buf[z, :, columns + k * LANES : columns + (k + 1) * LANES] = y_buf[k, :, columns:]
    copies = [send_small(z_buf.at[z], z_buf.at[z], 7 + k, p) for k, p in enumerate(z_peers)]
    for copy in copies:
        copy.wait_recv()
    scales[core, :, 0:columns] = jnp.maximum(
        jnp.maximum(z_buf[0, :, 0:columns], z_buf[1, :, 0:columns]),
        jnp.maximum(z_buf[2, :, 0:columns], z_buf[3, :, 0:columns]),
    )
    group = SIDE * LANES
    for k in range(SIDE):
        scales[core, :, columns + k * group : columns + (k + 1) * group] = z_buf[k, :, columns:]
    send_small(scales.at[core], scales.at[core], 10, partner).wait_recv()

    big = (big_g, big_u)
    own = pl.multiple_of(me * rows, rows)
    for a in (0, 1):

        @pl.loop(0, columns // LANES)
        def _(j):
            at = pl.ds(pl.multiple_of(j * LANES, LANES), LANES)
            factor = 1.0 / scales[a, :, at]
            big[a][pl.ds(own, rows), at] = (whole[a, :, at] * factor).astype(jnp.bfloat16)

    names = {}

    def number(chunk):
        return names.setdefault(chunk, len(names))

    def place(chunk, flip=False):
        array, first, second, cut = chunk
        dy, dz = (first, second) if array == 0 else (second, first)
        start = device(dz=dz, dy=dy, flip=flip) * rows + cut * part
        return pl.ds(pl.multiple_of(start, part), part)

    def pass_on(chunk, axis, step, turn):
        array, first, second, cut = chunk
        there = (array, *moved(first, second, turn, step), cut)
        piece = big[array].at[place(chunk)]
        copy = pltpu.make_async_remote_copy(
            src_ref=piece,
            dst_ref=piece,
            send_sem=ring_send.at[number(there)],
            recv_sem=ring_recv.at[number(there)],
            device_id=near(axis, step),
            device_id_type=MESH,
        )
        copy.start()
        sent.append(copy)

    def arrived(chunk):
        piece = big[chunk[0]].at[place(chunk)]
        pltpu.make_async_copy(piece, piece, ring_recv.at[number(chunk)]).wait()

    crossed = []

    def keep(chunk):
        array = chunk[0]
        piece = big[array].at[place(chunk)]
        copy = pltpu.make_async_remote_copy(
            src_ref=piece,
            dst_ref=piece,
            send_sem=core_send.at[len(crossed)],
            recv_sem=core_recv.at[len(crossed)],
            device_id=partner,
            device_id_type=MESH,
        )
        copy.start()
        sent.append(copy)
        crossed.append(chunk)

    taken = 0

    def take():
        chunk = crossed[taken]
        where = place(chunk, flip=True)
        piece = big[chunk[0]].at[where]
        pltpu.make_async_copy(piece, piece, core_recv.at[taken]).wait()

    for turn in (0, 1):
        for position in range(CUTS):
            for array in (0, 1):
                for axis, step, its_turn in onward(array, 0, 0, 0):
                    if its_turn == turn:
                        cut = position if step == 1 else CUTS - 1 - position
                        pass_on((array, 0, 0, cut), axis, step, turn)
    for cut in range(CUTS):
        for array in (0, 1):
            keep((array, 0, 0, cut))
    times = [0.0] * len(crossed)
    for now, chunk in arrivals():
        while taken < len(crossed) and times[taken] + 1.0 <= now:
            take()
            taken += 1
        arrived(chunk)
        for axis, step, turn in onward(*chunk):
            pass_on(chunk, axis, step, turn)
        keep(chunk)
        times.append(now)
    while taken < len(crossed):
        take()
        taken += 1
    for copy in sent:
        copy.wait_send()


def deliver(
    big_g, big_u, whole, scales,
    serving_g, serving_u, scale_g, scale_u, serve_norm, whole_g, whole_u, sem,
):
    columns = big_g.shape[1]
    copies = []

    def put(src, dst):
        copies.append(pltpu.make_async_copy(src, dst, sem.at[len(copies)]))
        copies[-1].start()

    step = big_g.shape[0] // PARTS
    for src, dst in ((big_g, serving_g), (big_u, serving_u)):
        for k in range(PARTS):
            put(src.at[pl.ds(k * step, step)], dst.at[pl.ds(k * step, step)])
    put(whole.at[0], whole_g)
    put(whole.at[1], whole_u)
    scale_g[...] = scales[0, :, 0:columns]
    scale_u[...] = scales[1, :, 0:columns]
    serve_norm[...] = (scales[0, :, columns:] + scales[1, :, columns:]).astype(jnp.bfloat16).reshape(-1)
    for copy in copies:
        copy.wait()


def body(wg, mg, sg, wu, mu, su, norm_train, norm_step):
    rows, columns = wg.shape
    total = rows * lax.axis_size("shard")
    chunks = 2 * CUTS * (SIDE * SIDE - 1)
    f32, bf16 = jnp.float32, jnp.bfloat16
    hbm, vmem = pl.BlockSpec(memory_space=pltpu.HBM), pl.BlockSpec(memory_space=pltpu.VMEM)
    dma = pltpu.SemaphoreType.DMA
    gathered = pl.pallas_call(
        kernel,
        out_shape=(
            pltpu.VMEM((total, columns), bf16),
            pltpu.VMEM((total, columns), bf16),
            pltpu.VMEM((2, rows, columns), f32),
            pltpu.VMEM((2, 1, columns + SIDE * SIDE * LANES), f32),
        ),
        in_specs=[hbm] * 8,
        out_specs=(vmem,) * 4,
        scratch_shapes=[
            pltpu.VMEM((2, rows, columns), f32),
            pltpu.VMEM((2, rows, columns), f32),
            pltpu.VMEM((2, rows, columns), f32),
            pltpu.VMEM((2, 1, columns), f32),
            pltpu.VMEM((1, columns), f32),
            pltpu.VMEM((SIDE, 1, columns + LANES), f32),
            pltpu.VMEM((SIDE, 1, columns + SIDE * LANES), f32),
            pltpu.VMEM((1, LANES), f32),
            pltpu.VMEM((SIDE, 1, LANES), f32),
            pltpu.VMEM((2, 1, 16), f32),
            dma((8,)),
            dma((11,)),
            dma((11,)),
            dma((chunks,)),
            dma((chunks,)),
            dma((chunks + 4 * CUTS,)),
            dma((chunks + 4 * CUTS,)),
        ],
        compiler_params=pltpu.CompilerParams(
            collective_id=0, has_side_effects=True, vmem_limit_bytes=47 * 1024 * 1024 - 300 * 1024
        ),
    )(wg, mg, sg, wu, mu, su, norm_train.reshape(1, -1), norm_step.reshape(1, -1))
    serving_g, serving_u, scale_g, scale_u, norm, whole_g, whole_u = pl.pallas_call(
        deliver,
        out_shape=(
            jax.ShapeDtypeStruct((total, columns), bf16),
            jax.ShapeDtypeStruct((total, columns), bf16),
            jax.ShapeDtypeStruct((1, columns), f32),
            jax.ShapeDtypeStruct((1, columns), f32),
            jax.ShapeDtypeStruct((total,), bf16),
            jax.ShapeDtypeStruct((rows, columns), f32),
            jax.ShapeDtypeStruct((rows, columns), f32),
        ),
        in_specs=[vmem] * 4,
        out_specs=(hbm, hbm, vmem, vmem, vmem, hbm, hbm),
        scratch_shapes=[dma((2 * PARTS + 2,))],
        compiler_params=pltpu.CompilerParams(vmem_limit_bytes=24 * 1024 * 1024),
    )(*gathered)
    return (
        serving_g,
        serving_u,
        scale_g.reshape(-1),
        scale_u.reshape(-1),
        norm,
        whole_g,
        whole_u,
    )


def solution(mesh):
    both = P("shard", "width")
    flat = P(("shard", "width"))
    wide = P(None, "width")
    return jax.shard_map(
        body,
        mesh=mesh,
        in_specs=(both,) * 6 + (flat, flat),
        out_specs=(wide, wide, P("width"), P("width"), P(), both, both),
        check_vma=False,
    )
```

```python
import heapq

import jax
import jax.numpy as jnp
from jax import lax
from jax.experimental import pallas as pl
from jax.experimental.pallas import tpu as pltpu
from jax.sharding import PartitionSpec as P

MESH = pl.DeviceIdType.MESH

learn_rate = 0.02
decay_rate = 0.1
tiny_value = 1e-08

SIDE = 4
CUTS = 2
LANES = 128
PARTS = 2


def axis_of(array, turn):
    return array if turn == 0 else 1 - array


def onward(array, first, second, cut):
    low = cut < CUTS // 2
    out = []
    if second == 0:
        if first == 0:
            out += [(0, 1), (0, -1)]
        elif first == -1 and low:
            out += [(0, 1)]
        elif first == 1 and not low:
            out += [(0, -1)]
        out += [(1, 1), (1, -1)]
    elif second == -1 and low:
        out += [(1, 1)]
    elif second == 1 and not low:
        out += [(1, -1)]
    return [(axis_of(array, turn), step, turn) for turn, step in out]


def moved(first, second, turn, step):
    def one(offset):
        return {0: -step, -step: 2}[offset]

    return (one(first), second) if turn == 0 else (first, one(second))


def early(array, step):
    return 0 if step == 1 else CUTS - 1


def starts():
    for turn in (0, 1):
        for position in range(CUTS):
            for array in (0, 1):
                for axis, step, its_turn in onward(array, 0, 0, 0):
                    cut = position if step == 1 else CUTS - 1 - position
                    if its_turn == turn and not (turn == 0 and cut == early(array, step)):
                        yield (array, 0, 0, cut), axis, step, turn


def arrivals():
    free = {}
    queue = []
    order = []
    span, delay = 1.0, 0.7

    def send(chunk, axis, step, turn, now):
        array, first, second, cut = chunk
        done = max(free.get((axis, step), 0.0), now) + span
        free[axis, step] = done
        heapq.heappush(queue, (done + delay, (array, *moved(first, second, turn, step), cut)))

    for chunk, axis, step, turn in starts():
        send(chunk, axis, step, turn, 0.0)
    for array in (0, 1):
        for step in (1, -1):
            heapq.heappush(queue, (0.0, (array, -step, 0, early(array, step))))
    while queue:
        now, chunk = heapq.heappop(queue)
        order.append((chunk, now == 0.0))
        for axis, step, turn in onward(*chunk):
            send(chunk, axis, step, turn, now)
    return order


def kernel(
    wg, mg, sg, wu, mu, su, norm_train, norm_step,
    big_g, big_u, whole, scales,
    w_in, m_in, s_in, local_max, y_buf, z_buf, ahead, norm_in, norm_row, norm_x, norm_y,
    in_sem, small_send, small_recv, ahead_send, ahead_recv, ring_send, ring_recv, core_sem,
):
    rows, columns = wg.shape
    part = rows // CUTS
    me, x = lax.axis_index("shard"), lax.axis_index("width")
    core = lax.rem(me, 2)
    y = lax.rem(lax.div(me, 2), SIDE)
    z = lax.div(me, 2 * SIDE)

    def device(dz=0, dy=0, flip=0):
        zz, yy = lax.rem(z + dz + SIDE, SIDE), lax.rem(y + dy + SIDE, SIDE)
        cc = 1 - core if flip else core
        return (zz * SIDE + yy) * 2 + cc

    def near(axis, step):
        return (device(dy=step) if axis == 0 else device(dz=step), x)

    partner = (device(flip=1), x)
    steps = [(k, flip) for k in (2, 1, 3) for flip in (0, 1)] + [(0, 1)]
    x_peers = [(me, lax.rem(x + k, SIDE)) for k in (1, 2, 3)]
    peers = (
        [(device(dy=k, flip=f), x) for k, f in steps]
        + [(device(dz=k, flip=f), x) for k, f in steps if k]
        + x_peers
    )

    inputs = ((wg, mg, sg), (wu, mu, su))
    loads = [
        [
            pltpu.make_async_copy(src, dst.at[a], in_sem.at[3 * a + k])
            for k, (src, dst) in enumerate(zip(inputs[a], (w_in, m_in, s_in)))
        ]
        for a in (0, 1)
    ]
    norms = [
        pltpu.make_async_copy(src, norm_in.at[k], in_sem.at[6 + k])
        for k, src in enumerate((norm_train, norm_step))
    ]
    for copy in loads[0] + loads[1] + norms:
        copy.start()

    barrier = pltpu.get_barrier_semaphore()
    for peer in peers:
        pl.semaphore_signal(barrier, inc=1, device_id=peer, device_id_type=MESH)

    for a in (0, 1):
        for copy in loads[a]:
            copy.wait()

        @pl.loop(0, columns // LANES)
        def _(j):
            at = pl.ds(pl.multiple_of(j * LANES, LANES), LANES)
            weight = w_in[a, :, at]
            new = weight - learn_rate * (
                m_in[a, :, at] / (jnp.sqrt(s_in[a, :, at]) + tiny_value) + decay_rate * weight
            )
            whole[a, :, at] = new
            local_max[a, :, at] = jnp.max(jnp.abs(new), axis=0, keepdims=True)

    for copy in norms:
        copy.wait()
    gain = norm_in[0] + norm_in[1]
    for k in range(8):
        norm_row[:, 16 * k : 16 * (k + 1)] = gain
    lane = lax.broadcasted_iota(jnp.int32, (1, LANES), 1)
    mine = lax.div(lane, 16) == core * SIDE + x
    norm_x[3] = jnp.where(mine, norm_row[...], 0.0)

    pl.semaphore_wait(barrier, len(peers))

    def send(src, dst, send_sem, recv_sem, peer):
        pltpu.make_async_remote_copy(
            src_ref=src,
            dst_ref=dst,
            send_sem=send_sem,
            recv_sem=recv_sem,
            device_id=peer,
            device_id_type=MESH,
        ).start()

    def small(stage, src, dst, peer):
        send(src, dst, small_send.at[stage], small_recv.at[stage], peer)

    def await_bytes(ref, sem):
        pltpu.make_async_copy(ref, ref, sem).wait()

    for k, flip in steps:
        a = 1 - core if flip else core
        small(0, local_max.at[a], y_buf.at[2 * ((SIDE - k) % SIDE) + flip - 1], (device(dy=k, flip=flip), x))

    def send_ahead(array, step, half):
        cut, slot = early(array, step), 2 * array + (step == -1)
        size = part // 2
        send(
            whole.at[array, pl.ds(cut * part + half * size, size)],
            ahead.at[slot, pl.ds(half * size, size)],
            ahead_send,
            ahead_recv.at[slot],
            near(array, step),
        )

    for step in (1, -1):
        send_ahead(1, step, 0)
    for half in (0, 1):
        for step in (1, -1):
            send_ahead(0, step, half)
    for k, peer in enumerate(x_peers):
        small(2, norm_x.at[3], norm_x.at[k], peer)
    await_bytes(y_buf, small_recv.at[0])
    best = local_max[core]
    for k in range(7):
        best = jnp.maximum(best, y_buf[k])
    await_bytes(norm_x.at[pl.ds(0, 3)], small_recv.at[2])
    here = SIDE * core + z
    z_buf[here, :, 0:columns] = best
    z_buf[here, :, columns:] = norm_x[0] + norm_x[1] + norm_x[2] + norm_x[3]
    for k, flip in steps:
        small(1, z_buf.at[here], z_buf.at[here], (device(dz=k, flip=flip), x))
    for step in (1, -1):
        send_ahead(1, step, 1)
    await_bytes(z_buf.at[pl.ds(0, 7)], small_recv.at[1])

    big = (big_g, big_u)
    own = pl.multiple_of(me * rows, rows)
    for a in (0, 1):
        first = SIDE * a

        @pl.loop(0, columns // LANES)
        def _(j):
            at = pl.ds(pl.multiple_of(j * LANES, LANES), LANES)
            best = jnp.maximum(
                jnp.maximum(z_buf[first, :, at], z_buf[first + 1, :, at]),
                jnp.maximum(z_buf[first + 2, :, at], z_buf[first + 3, :, at]),
            )
            scales[a, :, at] = best
            factor = 1.0 / best
            big[a][pl.ds(own, rows), at] = (whole[a, :, at] * factor).astype(jnp.bfloat16)

    for k in range(SIDE):
        norm_y[y, :, k * LANES : (k + 1) * LANES] = z_buf[k, :, columns:] + z_buf[SIDE + k, :, columns:]
    for k in (1, 2, 3):
        small(3, norm_y.at[y], norm_y.at[y], (device(dy=k), x))

    names = {}

    def number(chunk):
        return names.setdefault(chunk, len(names))

    def place(chunk):
        array, first, second, cut = chunk
        dy, dz = (first, second) if array == 0 else (second, first)
        start = device(dz=dz, dy=dy) * rows + cut * part
        return pl.ds(pl.multiple_of(start, part), part)

    def pass_on(chunk, axis, step, turn):
        array, first, second, cut = chunk
        there = (array, *moved(first, second, turn, step), cut)
        piece = big[array].at[place(chunk)]
        send(piece, piece, ring_send, ring_recv.at[number(there)], near(axis, step))

    def cross(chunk):
        piece = big[chunk[0]].at[place(chunk)]
        send(piece, piece, core_sem.at[0], core_sem.at[1], partner)

    for chunk, axis, step, turn in starts():
        pass_on(chunk, axis, step, turn)
    for array in (0, 1):
        for cut in range(CUTS):
            cross((array, 0, 0, cut))
    for chunk, came_early in arrivals():
        array, first, second, cut = chunk
        if came_early:
            slot = 2 * array + (first == 1)
            await_bytes(ahead.at[slot], ahead_recv.at[slot])
            where = place(chunk)

            @pl.loop(0, columns // LANES)
            def _(j):
                at = pl.ds(pl.multiple_of(j * LANES, LANES), LANES)
                factor = 1.0 / scales[array, :, at]
                big[array][where, at] = (ahead[slot, :, at] * factor).astype(jnp.bfloat16)

        else:
            await_bytes(big[array].at[place(chunk)], ring_recv.at[number(chunk)])
        for axis, step, turn in onward(*chunk):
            pass_on(chunk, axis, step, turn)
        cross(chunk)

    await_bytes(norm_y.at[pl.ds(0, 3)], small_recv.at[3])
    for k in range(SIDE):
        for i in range(SIDE):
            at = columns + (k * SIDE + i) * LANES
            scales[0, :, at : at + LANES] = norm_y[i, :, k * LANES : (k + 1) * LANES]
    await_bytes(y_buf, small_send.at[0])
    await_bytes(z_buf.at[pl.ds(0, 7)], small_send.at[1])
    await_bytes(norm_x.at[pl.ds(0, 3)], small_send.at[2])
    await_bytes(norm_y.at[pl.ds(0, 3)], small_send.at[3])
    await_bytes(whole, ahead_send)
    passed = 2 * CUTS * (SIDE * SIDE - 1) - 4
    await_bytes(big_g.at[pl.ds(0, passed * part)], ring_send)
    await_bytes(big_g, core_sem.at[0])
    await_bytes(big_u, core_sem.at[1])


def deliver(
    big_g, big_u, whole, scales,
    serving_g, serving_u, scale_g, scale_u, serve_norm, whole_g, whole_u, sem,
):
    columns = big_g.shape[1]
    copies = []

    def put(src, dst):
        copies.append(pltpu.make_async_copy(src, dst, sem.at[len(copies)]))
        copies[-1].start()

    step = big_g.shape[0] // PARTS
    for src, dst in ((big_g, serving_g), (big_u, serving_u)):
        for k in range(PARTS):
            put(src.at[pl.ds(k * step, step)], dst.at[pl.ds(k * step, step)])
    put(whole.at[0], whole_g)
    put(whole.at[1], whole_u)
    scale_g[...] = scales[0, :, 0:columns]
    scale_u[...] = scales[1, :, 0:columns]
    serve_norm[...] = scales[0, :, columns:].astype(jnp.bfloat16).reshape(-1)
    for copy in copies:
        copy.wait()


def body(wg, mg, sg, wu, mu, su, norm_train, norm_step):
    rows, columns = wg.shape
    total = rows * lax.axis_size("shard")
    chunks = 2 * CUTS * (SIDE * SIDE - 1) - 4
    f32, bf16 = jnp.float32, jnp.bfloat16
    hbm, vmem = pl.BlockSpec(memory_space=pltpu.HBM), pl.BlockSpec(memory_space=pltpu.VMEM)
    dma = pltpu.SemaphoreType.DMA
    gathered = pl.pallas_call(
        kernel,
        out_shape=(
            pltpu.VMEM((total, columns), bf16),
            pltpu.VMEM((total, columns), bf16),
            pltpu.VMEM((2, rows, columns), f32),
            pltpu.VMEM((2, 1, columns + SIDE * SIDE * LANES), f32),
        ),
        in_specs=[hbm] * 8,
        out_specs=(vmem,) * 4,
        scratch_shapes=[
            pltpu.VMEM((2, rows, columns), f32),
            pltpu.VMEM((2, rows, columns), f32),
            pltpu.VMEM((2, rows, columns), f32),
            pltpu.VMEM((2, 1, columns), f32),
            pltpu.VMEM((7, 1, columns), f32),
            pltpu.VMEM((2 * SIDE, 1, columns + LANES), f32),
            pltpu.VMEM((4, rows // CUTS, columns), f32),
            pltpu.VMEM((2, 1, 16), f32),
            pltpu.VMEM((1, LANES), f32),
            pltpu.VMEM((SIDE, 1, LANES), f32),
            pltpu.VMEM((SIDE, 1, SIDE * LANES), f32),
            dma((8,)),
            dma((4,)),
            dma((4,)),
            dma,
            dma((4,)),
            dma,
            dma((chunks,)),
            dma((2,)),
        ],
        compiler_params=pltpu.CompilerParams(
            collective_id=0, has_side_effects=True, vmem_limit_bytes=47 * 1024 * 1024 - 300 * 1024
        ),
    )(wg, mg, sg, wu, mu, su, norm_train.reshape(1, -1), norm_step.reshape(1, -1))
    serving_g, serving_u, scale_g, scale_u, norm, whole_g, whole_u = pl.pallas_call(
        deliver,
        out_shape=(
            jax.ShapeDtypeStruct((total, columns), bf16),
            jax.ShapeDtypeStruct((total, columns), bf16),
            jax.ShapeDtypeStruct((1, columns), f32),
            jax.ShapeDtypeStruct((1, columns), f32),
            jax.ShapeDtypeStruct((total,), bf16),
            jax.ShapeDtypeStruct((rows, columns), f32),
            jax.ShapeDtypeStruct((rows, columns), f32),
        ),
        in_specs=[vmem] * 4,
        out_specs=(hbm, hbm, vmem, vmem, vmem, hbm, hbm),
        scratch_shapes=[dma((2 * PARTS + 2,))],
        compiler_params=pltpu.CompilerParams(vmem_limit_bytes=24 * 1024 * 1024),
    )(*gathered)
    return (
        serving_g,
        serving_u,
        scale_g.reshape(-1),
        scale_u.reshape(-1),
        norm,
        whole_g,
        whole_u,
    )


def solution(mesh):
    both = P("shard", "width")
    flat = P(("shard", "width"))
    wide = P(None, "width")
    return jax.shard_map(
        body,
        mesh=mesh,
        in_specs=(both,) * 6 + (flat, flat),
        out_specs=(wide, wide, P("width"), P("width"), P(), both, both),
        check_vma=False,
    )
```

```python
import heapq

import jax
import jax.numpy as jnp
from jax import lax
from jax.experimental import pallas as pl
from jax.experimental.pallas import tpu as pltpu
from jax.sharding import PartitionSpec as P

MESH = pl.DeviceIdType.MESH

learn_rate = 0.02
decay_rate = 0.1
tiny_value = 1e-08

SIDE = 4
CUTS = 2
LANES = 128
PARTS = 2


def axis_of(array, turn):
    return array if turn == 0 else 1 - array


def onward(array, first, second, cut):
    low = cut < CUTS // 2
    out = []
    if second == 0:
        if first == 0:
            out += [(0, 1), (0, -1)]
        elif first == -1 and low:
            out += [(0, 1)]
        elif first == 1 and not low:
            out += [(0, -1)]
        out += [(1, 1), (1, -1)]
    elif second == -1 and low:
        out += [(1, 1)]
    elif second == 1 and not low:
        out += [(1, -1)]
    return [(axis_of(array, turn), step, turn) for turn, step in out]


def moved(first, second, turn, step):
    def one(offset):
        return {0: -step, -step: 2}[offset]

    return (one(first), second) if turn == 0 else (first, one(second))


def early(array, step):
    return 0 if step == 1 else CUTS - 1


def rest(array, step, part):
    return (part + part // 2, part // 2) if step == 1 else (0, part // 2)


def starts():
    for turn in (0, 1):
        for position in range(CUTS):
            for array in (0, 1):
                for axis, step, its_turn in onward(array, 0, 0, 0):
                    cut = position if step == 1 else CUTS - 1 - position
                    if its_turn == turn and not (turn == 0 and cut == early(array, step)):
                        yield (array, 0, 0, cut), axis, step, turn


def arrivals():
    free = {}
    queue = []
    order = []
    span, delay = 1.0, 0.7

    def send(chunk, axis, step, turn, now):
        array, first, second, cut = chunk
        own_rest = turn == 0 and first == 0
        done = max(free.get((axis, step), 0.0), now) + (span / 2 if own_rest else span)
        free[axis, step] = done
        heapq.heappush(queue, (done + delay, (array, *moved(first, second, turn, step), cut)))

    for chunk, axis, step, turn in starts():
        send(chunk, axis, step, turn, 0.0)
    for array in (0, 1):
        for step in (1, -1):
            heapq.heappush(queue, (0.0, (array, -step, 0, early(array, step))))
    while queue:
        now, chunk = heapq.heappop(queue)
        order.append((chunk, now == 0.0))
        for axis, step, turn in onward(*chunk):
            send(chunk, axis, step, turn, now)
    return order


def kernel(
    wg, mg, sg, wu, mu, su, norm_train, norm_step,
    big_g, big_u, whole, scales,
    loaded, local_max, y_buf, z_buf, ahead, norm_in, norm_row, norm_x, norm_y,
    in_sem, small_send, small_recv, ahead_send, ahead_recv, ring_send, ring_recv, core_sem,
):
    rows, columns = wg.shape
    part = rows // CUTS
    me, x = lax.axis_index("shard"), lax.axis_index("width")
    core = lax.rem(me, 2)
    y = lax.rem(lax.div(me, 2), SIDE)
    z = lax.div(me, 2 * SIDE)

    def device(dz=0, dy=0, flip=0):
        zz, yy = lax.rem(z + dz + SIDE, SIDE), lax.rem(y + dy + SIDE, SIDE)
        cc = 1 - core if flip else core
        return (zz * SIDE + yy) * 2 + cc

    def near(axis, step):
        return (device(dy=step) if axis == 0 else device(dz=step), x)

    partner = (device(flip=1), x)
    steps = [(k, flip) for k in (2, 1, 3) for flip in (0, 1)] + [(0, 1)]
    x_peers = [(me, lax.rem(x + k, SIDE)) for k in (1, 2, 3)]
    peers = (
        [(device(dy=k, flip=f), x) for k, f in steps]
        + [(device(dz=k, flip=f), x) for k, f in steps if k]
        + x_peers
    )

    half = columns // 2
    for a, refs in enumerate(((wg, mg, sg), (wu, mu, su))):
        for h in (0, 1):
            at = pl.ds(h * half, half)
            for k, src in enumerate(refs):
                pltpu.make_async_copy(src.at[:, at], loaded.at[k, a, :, at], in_sem.at[2 * a + h]).start()
    for k, src in enumerate((norm_train, norm_step)):
        pltpu.make_async_copy(src, norm_in.at[k], in_sem.at[4]).start()

    barrier = pltpu.get_barrier_semaphore()
    for peer in peers:
        pl.semaphore_signal(barrier, inc=1, device_id=peer, device_id_type=MESH)

    def await_bytes(ref, sem):
        pltpu.make_async_copy(ref, ref, sem).wait()

    for a in (0, 1):
        for h in (0, 1):
            await_bytes(loaded.at[:, a, :, pl.ds(h * half, half)], in_sem.at[2 * a + h])

            @pl.loop(0, half // LANES)
            def _(j):
                at = pl.ds(pl.multiple_of(h * half + j * LANES, LANES), LANES)
                weight, moment, square = (loaded[k, a, :, at] for k in range(3))
                new = weight - learn_rate * (
                    moment / (jnp.sqrt(square) + tiny_value) + decay_rate * weight
                )
                whole[a, :, at] = new
                local_max[a, :, at] = jnp.max(jnp.abs(new), axis=0, keepdims=True)

    await_bytes(norm_in, in_sem.at[4])
    gain = norm_in[0] + norm_in[1]
    for k in range(8):
        norm_row[:, 16 * k : 16 * (k + 1)] = gain
    lane = lax.broadcasted_iota(jnp.int32, (1, LANES), 1)
    mine = lax.div(lane, 16) == core * SIDE + x
    norm_x[3] = jnp.where(mine, norm_row[...], 0.0)

    pl.semaphore_wait(barrier, len(peers))

    def send(src, dst, send_sem, recv_sem, peer):
        pltpu.make_async_remote_copy(
            src_ref=src,
            dst_ref=dst,
            send_sem=send_sem,
            recv_sem=recv_sem,
            device_id=peer,
            device_id_type=MESH,
        ).start()

    def small(stage, src, dst, peer):
        send(src, dst, small_send.at[stage], small_recv.at[stage], peer)

    for k, flip in steps:
        a = 1 - core if flip else core
        small(0, local_max.at[a], y_buf.at[2 * ((SIDE - k) % SIDE) + flip - 1], (device(dy=k, flip=flip), x))

    def send_ahead(array, low, high, late):
        for step in (1, -1):
            side = int(step == -1)
            where = pl.ds(low if step == 1 else rows - high, high - low)
            send(
                whole.at[array, where],
                ahead.at[side, array, where],
                ahead_send,
                ahead_recv.at[2 * side + late],
                near(array, step),
            )

    send_ahead(1, 0, part // 2, 0)
    send_ahead(1, part // 2, 3 * part // 4, 0)
    send_ahead(0, 0, part, 0)
    send_ahead(0, part, 3 * part // 2, 1)
    for k, peer in enumerate(x_peers):
        small(2, norm_x.at[3], norm_x.at[k], peer)
    await_bytes(y_buf, small_recv.at[0])
    best = local_max[core]
    for k in range(7):
        best = jnp.maximum(best, y_buf[k])
    await_bytes(norm_x.at[pl.ds(0, 3)], small_recv.at[2])
    here = SIDE * core + z
    z_buf[here, :, 0:columns] = best
    z_buf[here, :, columns:] = norm_x[0] + norm_x[1] + norm_x[2] + norm_x[3]
    for k, flip in steps:
        small(1, z_buf.at[here], z_buf.at[here], (device(dz=k, flip=flip), x))
    send_ahead(1, 3 * part // 4, part, 0)
    send_ahead(1, part, 3 * part // 2, 1)
    await_bytes(z_buf.at[pl.ds(0, 7)], small_recv.at[1])

    big = (big_g, big_u)
    own = pl.multiple_of(me * rows, rows)

    def scaled(array, src, start, base, size, at):
        factor = 1.0 / scales[array, :, at]
        there = pl.ds(pl.multiple_of(base + start, size), size)
        big[array][there, at] = (src[pl.ds(start, size), at] * factor).astype(jnp.bfloat16)

    def blocks(work):
        @pl.loop(0, columns // LANES)
        def _(j):
            work(pl.ds(pl.multiple_of(j * LANES, LANES), LANES))

    def open_piece(at):
        for a in (0, 1):
            first = SIDE * a
            scales[a, :, at] = jnp.maximum(
                jnp.maximum(z_buf[first, :, at], z_buf[first + 1, :, at]),
                jnp.maximum(z_buf[first + 2, :, at], z_buf[first + 3, :, at]),
            )
            for step in (1, -1):
                start, size = rest(a, step, part)
                scaled(a, whole.at[a], start, own, size, at)

    def close_piece(at):
        for a in (0, 1):
            for start in (part // 2, part):
                scaled(a, whole.at[a], start, own, part // 2, at)

    blocks(open_piece)

    names = {}

    def arrival(first, second, cut, piece=0):
        return ring_recv.at[names.setdefault((first, second, cut, piece), len(names))]

    def start_of(array, first, second):
        dy, dz = (first, second) if array == 0 else (second, first)
        return device(dz=dz, dy=dy) * rows

    def span(array, first, second, start, size):
        at = start_of(array, first, second) + start
        return big[array].at[pl.ds(pl.multiple_of(at, size), size)]

    def parts_of(first, second, cut):
        pieces = 2 if first == 2 and second == 2 else 1
        size = part // pieces
        return [(cut * part + k * size, size) for k in range(pieces)]

    def pass_on(chunk, axis, step, turn):
        array, first, second, cut = chunk
        there = (*moved(first, second, turn, step), cut)
        copies = [rest(array, step, part)] if turn == 0 and first == 0 else parts_of(*there)
        for k, (start, size) in enumerate(copies):
            piece = span(array, first, second, start, size)
            send(piece, piece, ring_send, arrival(*there, k), near(axis, step))

    def cross(array, first, second, start, size):
        piece = span(array, first, second, start, size)
        send(piece, piece, core_sem.at[0], core_sem.at[1], partner)

    openings = list(starts())
    for chunk, axis, step, turn in openings:
        if turn == 0:
            pass_on(chunk, axis, step, turn)
    blocks(close_piece)
    for chunk, axis, step, turn in openings:
        if turn == 1:
            pass_on(chunk, axis, step, turn)
    for k in range(SIDE):
        norm_y[y, :, k * LANES : (k + 1) * LANES] = z_buf[k, :, columns:] + z_buf[SIDE + k, :, columns:]
    for k in (1, 2, 3):
        small(3, norm_y.at[y], norm_y.at[y], (device(dy=k), x))
    for array in (0, 1):
        for cut in range(CUTS):
            cross(array, 0, 0, cut * part, part)

    def from_ahead(side, first, start, size):
        def work(at):
            for array in (0, 1):
                scaled(array, ahead.at[side, array], start, start_of(array, first, 0), size, at)

        blocks(work)

    last = []
    for (array, first, second, cut), came_early in arrivals():
        if array == 1:
            continue
        if (first, second) == (2, 2):
            last.append(cut)
            continue
        side, size = int(first == 1), part // 2
        if came_early:
            await_bytes(ahead.at[side, :, pl.ds(0, part)], ahead_recv.at[2 * side])
            from_ahead(side, first, cut * part, part)
        elif second == 0 and first in (1, -1):
            await_bytes(ahead.at[side, :, pl.ds(0, size)], ahead_recv.at[2 * side + 1])
            from_ahead(side, first, size if first == 1 else part, size)
            await_bytes(big_g.at[pl.ds(0, 2 * size)], arrival(first, second, cut))
        else:
            await_bytes(big_g.at[pl.ds(0, 2 * part)], arrival(first, second, cut))
        for a in (0, 1):
            for axis, step, turn in onward(a, first, second, cut):
                pass_on((a, first, second, cut), axis, step, turn)
            cross(a, first, second, cut * part, part)
    for k in (0, 1):
        for cut in last:
            start, size = parts_of(2, 2, cut)[k]
            await_bytes(big_g.at[pl.ds(0, 2 * size)], arrival(2, 2, cut, k))
            for a in (0, 1):
                cross(a, 2, 2, start, size)

    await_bytes(norm_y.at[pl.ds(0, 3)], small_recv.at[3])
    for k in range(SIDE):
        for i in range(SIDE):
            at = columns + (k * SIDE + i) * LANES
            scales[0, :, at : at + LANES] = norm_y[i, :, k * LANES : (k + 1) * LANES]
    await_bytes(y_buf, small_send.at[0])
    await_bytes(z_buf.at[pl.ds(0, 7)], small_send.at[1])
    await_bytes(norm_x.at[pl.ds(0, 3)], small_send.at[2])
    await_bytes(norm_y.at[pl.ds(0, 3)], small_send.at[3])
    await_bytes(ahead.at[:, :, pl.ds(0, 3 * part // 2)], ahead_send)
    passed = 2 * CUTS * (SIDE * SIDE - 1) - 6
    await_bytes(big_g.at[pl.ds(0, passed * part)], ring_send)
    await_bytes(big_g, core_sem.at[0])
    await_bytes(big_u, core_sem.at[1])


def deliver(
    big_g, big_u, whole, scales,
    serving_g, serving_u, scale_g, scale_u, serve_norm, whole_g, whole_u, norm, sem,
):
    columns = big_g.shape[1]
    copies = []

    def put(src, dst):
        copies.append(pltpu.make_async_copy(src, dst, sem.at[len(copies)]))
        copies[-1].start()

    norm[...] = scales[0, :, columns:].astype(jnp.bfloat16).reshape(-1)
    put(scales.at[0, :, pl.ds(0, columns)], scale_g)
    put(scales.at[1, :, pl.ds(0, columns)], scale_u)
    put(whole.at[0], whole_g)
    put(whole.at[1], whole_u)
    step = big_g.shape[0] // PARTS
    for src, dst in ((big_g, serving_g), (big_u, serving_u)):
        for k in range(PARTS):
            put(src.at[pl.ds(k * step, step)], dst.at[pl.ds(k * step, step)])
    put(norm, serve_norm)
    for copy in copies:
        copy.wait()


def body(wg, mg, sg, wu, mu, su, norm_train, norm_step):
    rows, columns = wg.shape
    total = rows * lax.axis_size("shard")
    chunks = CUTS * (SIDE * SIDE - 1)
    f32, bf16 = jnp.float32, jnp.bfloat16
    hbm, vmem = pl.BlockSpec(memory_space=pltpu.HBM), pl.BlockSpec(memory_space=pltpu.VMEM)
    dma = pltpu.SemaphoreType.DMA
    gathered = pl.pallas_call(
        kernel,
        out_shape=(
            pltpu.VMEM((total, columns), bf16),
            pltpu.VMEM((total, columns), bf16),
            pltpu.VMEM((2, rows, columns), f32),
            pltpu.VMEM((2, 1, columns + SIDE * SIDE * LANES), f32),
        ),
        in_specs=[hbm] * 8,
        out_specs=(vmem,) * 4,
        scratch_shapes=[
            pltpu.VMEM((3, 2, rows, columns), f32),
            pltpu.VMEM((2, 1, columns), f32),
            pltpu.VMEM((7, 1, columns), f32),
            pltpu.VMEM((2 * SIDE, 1, columns + LANES), f32),
            pltpu.VMEM((2, 2, rows, columns), f32),
            pltpu.VMEM((2, 1, 16), f32),
            pltpu.VMEM((1, LANES), f32),
            pltpu.VMEM((SIDE, 1, LANES), f32),
            pltpu.VMEM((SIDE, 1, SIDE * LANES), f32),
            dma((5,)),
            dma((4,)),
            dma((4,)),
            dma,
            dma((4,)),
            dma,
            dma((chunks,)),
            dma((2,)),
        ],
        compiler_params=pltpu.CompilerParams(
            collective_id=0, has_side_effects=True, vmem_limit_bytes=47 * 1024 * 1024 - 300 * 1024
        ),
    )(wg, mg, sg, wu, mu, su, norm_train.reshape(1, -1), norm_step.reshape(1, -1))
    serving_g, serving_u, scale_g, scale_u, norm, whole_g, whole_u = pl.pallas_call(
        deliver,
        out_shape=(
            jax.ShapeDtypeStruct((total, columns), bf16),
            jax.ShapeDtypeStruct((total, columns), bf16),
            jax.ShapeDtypeStruct((1, columns), f32),
            jax.ShapeDtypeStruct((1, columns), f32),
            jax.ShapeDtypeStruct((total,), bf16),
            jax.ShapeDtypeStruct((rows, columns), f32),
            jax.ShapeDtypeStruct((rows, columns), f32),
        ),
        in_specs=[vmem] * 4,
        out_specs=(hbm,) * 7,
        scratch_shapes=[pltpu.VMEM((total,), bf16), dma((2 * PARTS + 5,))],
        compiler_params=pltpu.CompilerParams(vmem_limit_bytes=24 * 1024 * 1024),
    )(*gathered)
    return (
        serving_g,
        serving_u,
        scale_g.reshape(-1),
        scale_u.reshape(-1),
        norm,
        whole_g,
        whole_u,
    )


def solution(mesh):
    both = P("shard", "width")
    flat = P(("shard", "width"))
    wide = P(None, "width")
    return jax.shard_map(
        body,
        mesh=mesh,
        in_specs=(both,) * 6 + (flat, flat),
        out_specs=(wide, wide, P("width"), P("width"), P(), both, both),
        check_vma=False,
    )
```

```python
import heapq

import jax
import jax.numpy as jnp
from jax import lax
from jax.experimental import pallas as pl
from jax.experimental.pallas import tpu as pltpu
from jax.sharding import PartitionSpec as P

MESH = pl.DeviceIdType.MESH

learn_rate = 0.02
decay_rate = 0.1
tiny_value = 1e-08

SIDE = 4
CUTS = 2
LANES = 128
UNROLL = 4
PARTS = 2
AHEAD = 48
FIRST = 24
REST = 0.5


def axis_of(array, turn):
    return array if turn == 0 else 1 - array


def onward(array, first, second, cut):
    low = cut < CUTS // 2
    out = []
    if second == 0:
        if first == 0:
            out += [(0, 1), (0, -1)]
        elif first == -1 and low:
            out += [(0, 1)]
        elif first == 1 and not low:
            out += [(0, -1)]
        out += [(1, 1), (1, -1)]
    elif second == -1 and low:
        out += [(1, 1)]
    elif second == 1 and not low:
        out += [(1, -1)]
    return [(axis_of(array, turn), step, turn) for turn, step in out]


def moved(first, second, turn, step):
    def one(offset):
        return {0: -step, -step: 2}[offset]

    return (one(first), second) if turn == 0 else (first, one(second))


def early(array, step):
    return 0 if step == 1 else CUTS - 1


def rest(array, step, part):
    return (AHEAD, 2 * part - AHEAD) if step == 1 else (0, 2 * part - AHEAD)


def starts():
    for turn in (0, 1):
        for position in range(CUTS):
            for array in (0, 1):
                for axis, step, its_turn in onward(array, 0, 0, 0):
                    cut = position if step == 1 else CUTS - 1 - position
                    if its_turn == turn and not (turn == 0 and cut == early(array, step)):
                        yield (array, 0, 0, cut), axis, step, turn


def arrivals():
    free = {}
    queue = []
    order = []
    span, delay = 1.0, 0.7

    def send(chunk, axis, step, turn, now):
        array, first, second, cut = chunk
        own_rest = turn == 0 and first == 0
        done = max(free.get((axis, step), 0.0), now) + (REST if own_rest else span)
        free[axis, step] = done
        heapq.heappush(queue, (done + delay, (array, *moved(first, second, turn, step), cut)))

    for chunk, axis, step, turn in starts():
        send(chunk, axis, step, turn, 0.0)
    for array in (0, 1):
        for step in (1, -1):
            heapq.heappush(queue, (0.0, (array, -step, 0, early(array, step))))
    while queue:
        now, chunk = heapq.heappop(queue)
        order.append((chunk, now == 0.0))
        for axis, step, turn in onward(*chunk):
            send(chunk, axis, step, turn, now)
    return order


def kernel(
    wg, mg, sg, wu, mu, su, norm_train, norm_step,
    big_g, big_u, whole, scales,
    loaded, local_max, y_buf, z_buf, ahead, norm_in, norm_row, norm_z, norm_x, norm_y,
    in_sem, small_send, small_recv, norm_send, norm_recv, ahead_send, ahead_recv, ring_send, ring_recv, core_sem,
):
    rows, columns = wg.shape
    part = rows // CUTS
    me, x = lax.axis_index("shard"), lax.axis_index("width")
    core = lax.rem(me, 2)
    y = lax.rem(lax.div(me, 2), SIDE)
    z = lax.div(me, 2 * SIDE)

    def device(dz=0, dy=0, flip=0):
        zz, yy = lax.rem(z + dz + SIDE, SIDE), lax.rem(y + dy + SIDE, SIDE)
        cc = 1 - core if flip else core
        return (zz * SIDE + yy) * 2 + cc

    def near(axis, step):
        return (device(dy=step) if axis == 0 else device(dz=step), x)

    partner = (device(flip=1), x)
    steps = [(k, flip) for k in (2, 1, 3) for flip in (0, 1)] + [(0, 1)]
    x_peers = [(me, lax.rem(x + k, SIDE)) for k in (1, 2, 3)]
    y_peers = [(device(dy=k, flip=f), x) for k, f in steps]
    z_peers = [(device(dz=k, flip=f), x) for k, f in steps]
    peers = y_peers + z_peers[:-1]

    half = columns // 2
    for a, refs in enumerate(((wg, mg, sg), (wu, mu, su))):
        for h in (0, 1):
            at = pl.ds(h * half, half)
            for k, src in enumerate(refs):
                pltpu.make_async_copy(src.at[:, at], loaded.at[k, a, :, at], in_sem.at[2 * a + h]).start()
    for k, src in enumerate((norm_train, norm_step)):
        pltpu.make_async_copy(src, norm_in.at[k], in_sem.at[4]).start()

    barrier = pltpu.get_barrier_semaphore()
    for peer in peers:
        pl.semaphore_signal(barrier, inc=1, device_id=peer, device_id_type=MESH)

    @pl.when(z == 0)
    def _():
        for peer in x_peers:
            pl.semaphore_signal(barrier, inc=1, device_id=peer, device_id_type=MESH)

    def await_bytes(ref, sem):
        pltpu.make_async_copy(ref, ref, sem).wait()

    for a in (0, 1):
        for h in (0, 1):
            await_bytes(loaded.at[:, a, :, pl.ds(h * half, half)], in_sem.at[2 * a + h])

            @pl.loop(0, half // LANES, unroll=UNROLL)
            def _(j):
                at = pl.ds(pl.multiple_of(h * half + j * LANES, LANES), LANES)
                weight, moment, square = (loaded[k, a, :, at] for k in range(3))
                root = square * lax.rsqrt(square) + tiny_value
                new = weight * (1.0 - learn_rate * decay_rate) - (learn_rate * moment) / root
                whole[a, :, at] = new
                local_max[a, :, at] = jnp.max(jnp.abs(new), axis=0, keepdims=True)

    await_bytes(norm_in, in_sem.at[4])
    gain = norm_in[0] + norm_in[1]
    for k in range(8):
        norm_row[:, 16 * k : 16 * (k + 1)] = gain
    lane = lax.broadcasted_iota(jnp.int32, (1, LANES), 1)
    mine = lax.div(lane, 16) == core * SIDE + x
    norm_z[z] = jnp.where(mine, norm_row[...], 0.0)

    pl.semaphore_wait(barrier, len(peers) + len(x_peers) * lax.div(SIDE - z, SIDE))

    def send(src, dst, send_sem, recv_sem, peer):
        pltpu.make_async_remote_copy(
            src_ref=src,
            dst_ref=dst,
            send_sem=send_sem,
            recv_sem=recv_sem,
            device_id=peer,
            device_id_type=MESH,
        ).start()

    def small(stage, src, dst, peer):
        send(src, dst, small_send.at[stage], small_recv.at[stage], peer)

    for k, flip in steps:
        a = 1 - core if flip else core
        small(0, local_max.at[a], y_buf.at[2 * ((SIDE - k) % SIDE) + flip - 1], (device(dy=k, flip=flip), x))

    def gain(stage, src, dst, peer):
        send(src, dst, norm_send.at[stage], norm_recv.at[stage], peer)

    norm_whole = scales.at[0, :, pl.ds(columns, SIDE * SIDE * LANES)]

    def gain_over_x():
        @pl.when(z == 0)
        def _():
            await_bytes(norm_z.at[pl.ds(0, 3)], norm_recv.at[0])
            for k, peer in enumerate(x_peers):
                gain(1, norm_z, norm_x.at[k], peer)

    def gain_over_y():
        @pl.when(z == 0)
        def _():
            await_bytes(norm_x, norm_recv.at[1])
            slot = SIDE * core + y
            norm_y[slot] = norm_z[...] + norm_x[0] + norm_x[1] + norm_x[2]
            for peer in y_peers:
                gain(2, norm_y.at[slot], norm_y.at[slot], peer)

    def gain_over_z():
        @pl.when(z == 0)
        def _():
            await_bytes(norm_y.at[pl.ds(0, 7)], norm_recv.at[2])
            for k in range(SIDE):
                for i in range(SIDE):
                    at = columns + (k * SIDE + i) * LANES
                    scales[0, :, at : at + LANES] = norm_y[i, k] + norm_y[SIDE + i, k]
            for k in (1, 2, 3):
                gain(3, norm_whole, norm_whole, (device(dz=k), x))

    @pl.when(z > 0)
    def _():
        gain(0, norm_z.at[z], norm_z.at[z], (device(dz=-z), x))

    def send_ahead(array, low, high, late):
        for step in (1, -1):
            side = int(step == -1)
            where = pl.ds(low if step == 1 else rows - high, high - low)
            send(
                whole.at[array, where],
                ahead.at[side, array, where],
                ahead_send,
                ahead_recv.at[2 * side + late],
                near(array, step),
            )

    send_ahead(1, 0, FIRST, 0)
    send_ahead(0, 0, part, 0)
    send_ahead(0, part, AHEAD, 1)
    await_bytes(y_buf, small_recv.at[0])
    best = local_max[core]
    for k in range(7):
        best = jnp.maximum(best, y_buf[k])
    here = SIDE * core + z
    z_buf[here] = best
    for k, flip in steps:
        small(1, z_buf.at[here], z_buf.at[here], (device(dz=k, flip=flip), x))
    send_ahead(1, FIRST, part, 0)
    send_ahead(1, part, AHEAD, 1)
    await_bytes(z_buf.at[pl.ds(0, 7)], small_recv.at[1])

    big = (big_g, big_u)
    own = pl.multiple_of(me * rows, rows)

    def scaled(array, src, start, base, size, at):
        factor = 1.0 / scales[array, :, at]
        there = pl.ds(pl.multiple_of(base + start, 8), size)
        big[array][there, at] = (src[pl.ds(start, size), at] * factor).astype(jnp.bfloat16)

    def blocks(work):
        @pl.loop(0, columns // LANES, unroll=UNROLL)
        def _(j):
            work(pl.ds(pl.multiple_of(j * LANES, LANES), LANES))

    def open_piece(at):
        for a in (0, 1):
            first = SIDE * a
            scales[a, :, at] = jnp.maximum(
                jnp.maximum(z_buf[first, :, at], z_buf[first + 1, :, at]),
                jnp.maximum(z_buf[first + 2, :, at], z_buf[first + 3, :, at]),
            )
            for step in (1, -1):
                start, size = rest(a, step, part)
                scaled(a, whole.at[a], start, own, size, at)

    def close_piece(at):
        for a in (0, 1):
            scaled(a, whole.at[a], 2 * part - AHEAD, own, 2 * AHEAD - 2 * part, at)

    blocks(open_piece)

    names = {}

    def arrival(first, second, cut, piece=0):
        return ring_recv.at[names.setdefault((first, second, cut, piece), len(names))]

    def start_of(array, first, second):
        dy, dz = (first, second) if array == 0 else (second, first)
        return device(dz=dz, dy=dy) * rows

    def span(array, first, second, start, size):
        at = start_of(array, first, second) + start
        return big[array].at[pl.ds(pl.multiple_of(at, 8), size)]

    def parts_of(first, second, cut):
        pieces = 2 if first == 2 and second == 2 else 1
        size = part // pieces
        return [(cut * part + k * size, size) for k in range(pieces)]

    def pass_on(chunk, axis, step, turn):
        array, first, second, cut = chunk
        there = (*moved(first, second, turn, step), cut)
        copies = [rest(array, step, part)] if turn == 0 and first == 0 else parts_of(*there)
        for k, (start, size) in enumerate(copies):
            piece = span(array, first, second, start, size)
            send(piece, piece, ring_send, arrival(*there, k), near(axis, step))

    def cross(array, first, second, start, size):
        piece = span(array, first, second, start, size)
        send(piece, piece, core_sem.at[0], core_sem.at[1], partner)

    openings = list(starts())
    for chunk, axis, step, turn in openings:
        if turn == 0:
            pass_on(chunk, axis, step, turn)
    blocks(close_piece)
    for chunk, axis, step, turn in openings:
        if turn == 1:
            pass_on(chunk, axis, step, turn)
    gain_over_x()
    for array in (0, 1):
        for cut in range(CUTS):
            cross(array, 0, 0, cut * part, part)

    def from_ahead(side, first, start, size):
        def work(at):
            for array in (0, 1):
                scaled(array, ahead.at[side, array], start, start_of(array, first, 0), size, at)

        blocks(work)

    last = []
    for (array, first, second, cut), came_early in arrivals():
        if array == 1:
            continue
        if (first, second) == (2, 2):
            last.append(cut)
            continue
        side, size, left = int(first == 1), AHEAD - part, 2 * part - AHEAD
        if came_early:
            await_bytes(ahead.at[side, :, pl.ds(0, part)], ahead_recv.at[2 * side])
            from_ahead(side, first, cut * part, part)
        elif second == 0 and first in (1, -1):
            await_bytes(ahead.at[side, :, pl.ds(0, size)], ahead_recv.at[2 * side + 1])
            from_ahead(side, first, left if first == 1 else part, size)
            await_bytes(big_g.at[pl.ds(0, 2 * left)], arrival(first, second, cut))
            if first == 1:
                gain_over_y()
        else:
            await_bytes(big_g.at[pl.ds(0, 2 * part)], arrival(first, second, cut))
        for a in (0, 1):
            for axis, step, turn in onward(a, first, second, cut):
                pass_on((a, first, second, cut), axis, step, turn)
            cross(a, first, second, cut * part, part)
        if (first, second, cut) == (-1, 1, 1):
            gain_over_z()
    for k in (0, 1):
        for cut in last:
            start, size = parts_of(2, 2, cut)[k]
            await_bytes(big_g.at[pl.ds(0, 2 * size)], arrival(2, 2, cut, k))
            for a in (0, 1):
                cross(a, 2, 2, start, size)

    @pl.when(z > 0)
    def _():
        await_bytes(norm_whole, norm_recv.at[3])
        await_bytes(norm_z.at[0], norm_send.at[0])

    @pl.when(z == 0)
    def _():
        await_bytes(norm_x, norm_send.at[1])
        await_bytes(norm_y.at[pl.ds(0, 7)], norm_send.at[2])
        await_bytes(y_buf.at[pl.ds(0, 3)], norm_send.at[3])

    await_bytes(y_buf, small_send.at[0])
    await_bytes(z_buf.at[pl.ds(0, 7)], small_send.at[1])
    await_bytes(ahead.at[:, :, pl.ds(0, AHEAD)], ahead_send)
    passed = 2 * (SIDE * SIDE - 1) * rows - 4 * AHEAD
    await_bytes(big_g.at[pl.ds(0, passed)], ring_send)
    await_bytes(big_g, core_sem.at[0])
    await_bytes(big_u, core_sem.at[1])


def deliver(
    big_g, big_u, whole, scales,
    serving_g, serving_u, scale_g, scale_u, serve_norm, whole_g, whole_u, norm, sem,
):
    columns = big_g.shape[1]
    copies = []

    def put(src, dst):
        copies.append(pltpu.make_async_copy(src, dst, sem.at[len(copies)]))
        copies[-1].start()

    step = big_g.shape[0] // PARTS
    for src, dst in ((big_g, serving_g), (big_u, serving_u)):
        for k in range(PARTS):
            put(src.at[pl.ds(k * step, step)], dst.at[pl.ds(k * step, step)])
    put(whole.at[0], whole_g)
    put(whole.at[1], whole_u)
    put(scales.at[0, :, pl.ds(0, columns)], scale_g)
    put(scales.at[1, :, pl.ds(0, columns)], scale_u)
    norm[...] = scales[0, :, columns:].astype(jnp.bfloat16).reshape(-1)
    put(norm, serve_norm)
    for copy in copies:
        copy.wait()


def body(wg, mg, sg, wu, mu, su, norm_train, norm_step):
    rows, columns = wg.shape
    total = rows * lax.axis_size("shard")
    chunks = CUTS * (SIDE * SIDE - 1)
    f32, bf16 = jnp.float32, jnp.bfloat16
    hbm, vmem = pl.BlockSpec(memory_space=pltpu.HBM), pl.BlockSpec(memory_space=pltpu.VMEM)
    dma = pltpu.SemaphoreType.DMA
    gathered = pl.pallas_call(
        kernel,
        out_shape=(
            pltpu.VMEM((total, columns), bf16),
            pltpu.VMEM((total, columns), bf16),
            pltpu.VMEM((2, rows, columns), f32),
            pltpu.VMEM((2, 1, columns + SIDE * SIDE * LANES), f32),
        ),
        in_specs=[hbm] * 8,
        out_specs=(vmem,) * 4,
        scratch_shapes=[
            pltpu.VMEM((3, 2, rows, columns), f32),
            pltpu.VMEM((2, 1, columns), f32),
            pltpu.VMEM((7, 1, columns), f32),
            pltpu.VMEM((2 * SIDE, 1, columns), f32),
            pltpu.VMEM((2, 2, rows, columns), f32),
            pltpu.VMEM((2, 1, 16), f32),
            pltpu.VMEM((1, LANES), f32),
            pltpu.VMEM((SIDE, 1, LANES), f32),
            pltpu.VMEM((3, SIDE, 1, LANES), f32),
            pltpu.VMEM((2 * SIDE, SIDE, 1, LANES), f32),
            dma((5,)),
            dma((2,)),
            dma((2,)),
            dma((4,)),
            dma((4,)),
            dma,
            dma((4,)),
            dma,
            dma((chunks,)),
            dma((2,)),
        ],
        compiler_params=pltpu.CompilerParams(
            collective_id=0, has_side_effects=True, vmem_limit_bytes=47 * 1024 * 1024 - 300 * 1024
        ),
    )(wg, mg, sg, wu, mu, su, norm_train.reshape(1, -1), norm_step.reshape(1, -1))
    serving_g, serving_u, scale_g, scale_u, norm, whole_g, whole_u = pl.pallas_call(
        deliver,
        out_shape=(
            jax.ShapeDtypeStruct((total, columns), bf16),
            jax.ShapeDtypeStruct((total, columns), bf16),
            jax.ShapeDtypeStruct((1, columns), f32),
            jax.ShapeDtypeStruct((1, columns), f32),
            jax.ShapeDtypeStruct((total,), bf16),
            jax.ShapeDtypeStruct((rows, columns), f32),
            jax.ShapeDtypeStruct((rows, columns), f32),
        ),
        in_specs=[vmem] * 4,
        out_specs=(hbm,) * 7,
        scratch_shapes=[pltpu.VMEM((total,), bf16), dma((2 * PARTS + 5,))],
        compiler_params=pltpu.CompilerParams(vmem_limit_bytes=24 * 1024 * 1024),
    )(*gathered)
    return (
        serving_g,
        serving_u,
        scale_g.reshape(-1),
        scale_u.reshape(-1),
        norm,
        whole_g,
        whole_u,
    )


def solution(mesh):
    both = P("shard", "width")
    flat = P(("shard", "width"))
    wide = P(None, "width")
    return jax.shard_map(
        body,
        mesh=mesh,
        in_specs=(both,) * 6 + (flat, flat),
        out_specs=(wide, wide, P("width"), P("width"), P(), both, both),
        check_vma=False,
    )
```

```python
import heapq

import jax
import jax.numpy as jnp
from jax import lax
from jax.experimental import pallas as pl
from jax.experimental.pallas import tpu as pltpu
from jax.sharding import PartitionSpec as P

MESH = pl.DeviceIdType.MESH

learn_rate = 0.02
decay_rate = 0.1
tiny_value = 1e-08

SIDE = 4
CUTS = 2
LANES = 128
UNROLL = 4
PARTS = 2
AHEAD = 48
FIRST = 24
REST = 0.5


def axis_of(array, turn):
    return array if turn == 0 else 1 - array


def onward(array, first, second, cut):
    low = cut < CUTS // 2
    out = []
    if second == 0:
        if first == 0:
            out += [(0, 1), (0, -1)]
        elif first == -1 and low:
            out += [(0, 1)]
        elif first == 1 and not low:
            out += [(0, -1)]
        out += [(1, 1), (1, -1)]
    elif second == -1 and low:
        out += [(1, 1)]
    elif second == 1 and not low:
        out += [(1, -1)]
    return [(axis_of(array, turn), step, turn) for turn, step in out]


def moved(first, second, turn, step):
    def one(offset):
        return {0: -step, -step: 2}[offset]

    return (one(first), second) if turn == 0 else (first, one(second))


def early(array, step):
    return 0 if step == 1 else CUTS - 1


def rest(array, step, part):
    return (AHEAD, 2 * part - AHEAD) if step == 1 else (0, 2 * part - AHEAD)


def starts():
    for turn in (0, 1):
        for position in range(CUTS):
            for array in (0, 1):
                for axis, step, its_turn in onward(array, 0, 0, 0):
                    cut = position if step == 1 else CUTS - 1 - position
                    if its_turn == turn and not (turn == 0 and cut == early(array, step)):
                        yield (array, 0, 0, cut), axis, step, turn


def arrivals():
    free = {}
    queue = []
    order = []
    span, delay = 1.0, 0.7

    def send(chunk, axis, step, turn, now):
        array, first, second, cut = chunk
        own_rest = turn == 0 and first == 0
        done = max(free.get((axis, step), 0.0), now) + (REST if own_rest else span)
        free[axis, step] = done
        heapq.heappush(queue, (done + delay, (array, *moved(first, second, turn, step), cut)))

    for chunk, axis, step, turn in starts():
        send(chunk, axis, step, turn, 0.0)
    for array in (0, 1):
        for step in (1, -1):
            heapq.heappush(queue, (0.0, (array, -step, 0, early(array, step))))
    while queue:
        now, chunk = heapq.heappop(queue)
        order.append((chunk, now == 0.0))
        for axis, step, turn in onward(*chunk):
            send(chunk, axis, step, turn, now)
    return order


def kernel(
    wg, mg, sg, wu, mu, su, norm_train, norm_step,
    big_g, big_u, whole, scales,
    loaded, local_max, y_buf, z_buf, ahead, norm_in, norm_row, norm_z, norm_x, norm_y,
    in_sem, small_send, small_recv, norm_send, norm_recv, ahead_send, ahead_recv, ring_send, ring_recv, core_sem,
):
    rows, columns = wg.shape
    part = rows // CUTS
    me, x = lax.axis_index("shard"), lax.axis_index("width")
    core = lax.rem(me, 2)
    y = lax.rem(lax.div(me, 2), SIDE)
    z = lax.div(me, 2 * SIDE)

    def device(dz=0, dy=0, flip=0):
        zz, yy = lax.rem(z + dz + SIDE, SIDE), lax.rem(y + dy + SIDE, SIDE)
        cc = 1 - core if flip else core
        return (zz * SIDE + yy) * 2 + cc

    def near(axis, step):
        return (device(dy=step) if axis == 0 else device(dz=step), x)

    partner = (device(flip=1), x)
    steps = [(k, flip) for k in (2, 1, 3) for flip in (0, 1)] + [(0, 1)]
    x_peers = [(me, lax.rem(x + k, SIDE)) for k in (1, 2, 3)]
    y_peers = [(device(dy=k, flip=f), x) for k, f in steps]
    z_peers = [(device(dz=k, flip=f), x) for k, f in steps]
    peers = y_peers + z_peers[:-1]

    half = columns // 2
    for a, refs in enumerate(((wg, mg, sg), (wu, mu, su))):
        for h in (0, 1):
            at = pl.ds(h * half, half)
            for k, src in enumerate(refs):
                pltpu.make_async_copy(src.at[:, at], loaded.at[k, a, :, at], in_sem.at[2 * a + h]).start()
    for k, src in enumerate((norm_train, norm_step)):
        pltpu.make_async_copy(src, norm_in.at[k], in_sem.at[4]).start()

    barrier = pltpu.get_barrier_semaphore()
    for peer in peers:
        pl.semaphore_signal(barrier, inc=1, device_id=peer, device_id_type=MESH)

    @pl.when(z == 0)
    def _():
        for peer in x_peers:
            pl.semaphore_signal(barrier, inc=1, device_id=peer, device_id_type=MESH)

    def await_bytes(ref, sem):
        pltpu.make_async_copy(ref, ref, sem).wait()

    for a in (0, 1):
        for h in (0, 1):
            await_bytes(loaded.at[:, a, :, pl.ds(h * half, half)], in_sem.at[2 * a + h])

            @pl.loop(0, half // LANES, unroll=UNROLL)
            def _(j):
                at = pl.ds(pl.multiple_of(h * half + j * LANES, LANES), LANES)
                weight, moment, square = (loaded[k, a, :, at] for k in range(3))
                root = square * lax.rsqrt(square) + tiny_value
                new = weight * (1.0 - learn_rate * decay_rate) - (learn_rate * moment) / root
                whole[a, :, at] = new
                local_max[a, :, at] = jnp.max(jnp.abs(new), axis=0, keepdims=True)

    await_bytes(norm_in, in_sem.at[4])
    gain = norm_in[0] + norm_in[1]
    for k in range(8):
        norm_row[:, 16 * k : 16 * (k + 1)] = gain
    lane = lax.broadcasted_iota(jnp.int32, (1, LANES), 1)
    mine = lax.div(lane, 16) == core * SIDE + x
    norm_z[z] = jnp.where(mine, norm_row[...], 0.0)

    pl.semaphore_wait(barrier, len(peers) + len(x_peers) * lax.div(SIDE - z, SIDE))

    def send(src, dst, send_sem, recv_sem, peer):
        pltpu.make_async_remote_copy(
            src_ref=src,
            dst_ref=dst,
            send_sem=send_sem,
            recv_sem=recv_sem,
            device_id=peer,
            device_id_type=MESH,
        ).start()

    def small(stage, src, dst, peer):
        send(src, dst, small_send.at[stage], small_recv.at[stage], peer)

    for k, flip in steps:
        a = 1 - core if flip else core
        small(0, local_max.at[a], y_buf.at[2 * ((SIDE - k) % SIDE) + flip - 1], (device(dy=k, flip=flip), x))

    def gain(stage, src, dst, peer):
        send(src, dst, norm_send.at[stage], norm_recv.at[stage], peer)

    norm_whole = scales.at[0, :, pl.ds(columns, SIDE * SIDE * LANES)]

    def gain_over_x():
        @pl.when(z == 0)
        def _():
            await_bytes(norm_z.at[pl.ds(0, 3)], norm_recv.at[0])
            for k, peer in enumerate(x_peers):
                gain(1, norm_z, norm_x.at[k], peer)

    def gain_over_y():
        @pl.when(z == 0)
        def _():
            await_bytes(norm_x, norm_recv.at[1])
            slot = SIDE * core + y
            norm_y[slot] = norm_z[...] + norm_x[0] + norm_x[1] + norm_x[2]
            for peer in y_peers:
                gain(2, norm_y.at[slot], norm_y.at[slot], peer)

    def gain_over_z():
        @pl.when(z == 0)
        def _():
            await_bytes(norm_y.at[pl.ds(0, 7)], norm_recv.at[2])
            for k in range(SIDE):
                for i in range(SIDE):
                    at = columns + (k * SIDE + i) * LANES
                    scales[0, :, at : at + LANES] = norm_y[i, k] + norm_y[SIDE + i, k]
            for k in (1, 2, 3):
                gain(3, norm_whole, norm_whole, (device(dz=k), x))

    @pl.when(z > 0)
    def _():
        gain(0, norm_z.at[z], norm_z.at[z], (device(dz=-z), x))

    def send_ahead(array, low, high, late):
        for step in (1, -1):
            side = int(step == -1)
            where = pl.ds(low if step == 1 else rows - high, high - low)
            send(
                whole.at[array, where],
                ahead.at[side, array, where],
                ahead_send,
                ahead_recv.at[2 * side + late],
                near(array, step),
            )

    send_ahead(1, 0, FIRST, 0)
    send_ahead(0, 0, part, 0)
    send_ahead(0, part, AHEAD, 1)
    await_bytes(y_buf, small_recv.at[0])
    best = local_max[core]
    for k in range(7):
        best = jnp.maximum(best, y_buf[k])
    here = SIDE * core + z
    z_buf[here] = best
    for k, flip in steps:
        small(1, z_buf.at[here], z_buf.at[here], (device(dz=k, flip=flip), x))
    send_ahead(1, FIRST, part, 0)
    send_ahead(1, part, AHEAD, 1)
    await_bytes(z_buf.at[pl.ds(0, 7)], small_recv.at[1])

    big = (big_g, big_u)
    own = pl.multiple_of(me * rows, rows)

    def scaled(array, src, start, base, size, at):
        factor = 1.0 / scales[array, :, at]
        there = pl.ds(pl.multiple_of(base + start, 8), size)
        big[array][there, at] = (src[pl.ds(start, size), at] * factor).astype(jnp.bfloat16)

    def blocks(work):
        @pl.loop(0, columns // LANES, unroll=UNROLL)
        def _(j):
            work(pl.ds(pl.multiple_of(j * LANES, LANES), LANES))

    def open_piece(at):
        for a in (0, 1):
            first = SIDE * a
            scales[a, :, at] = jnp.maximum(
                jnp.maximum(z_buf[first, :, at], z_buf[first + 1, :, at]),
                jnp.maximum(z_buf[first + 2, :, at], z_buf[first + 3, :, at]),
            )
            for step in (1, -1):
                start, size = rest(a, step, part)
                scaled(a, whole.at[a], start, own, size, at)

    def close_piece(at):
        for a in (0, 1):
            scaled(a, whole.at[a], 2 * part - AHEAD, own, 2 * AHEAD - 2 * part, at)

    blocks(open_piece)

    names = {}

    def arrival(first, second, cut, piece=0):
        return ring_recv.at[names.setdefault((first, second, cut, piece), len(names))]

    def start_of(array, first, second):
        dy, dz = (first, second) if array == 0 else (second, first)
        return device(dz=dz, dy=dy) * rows

    def span(array, first, second, start, size):
        at = start_of(array, first, second) + start
        return big[array].at[pl.ds(pl.multiple_of(at, 8), size)]

    def parts_of(first, second, cut):
        pieces = 2 if first == 2 and second == 2 else 1
        size = part // pieces
        return [(cut * part + k * size, size) for k in range(pieces)]

    def pass_on(chunk, axis, step, turn):
        array, first, second, cut = chunk
        there = (*moved(first, second, turn, step), cut)
        copies = [rest(array, step, part)] if turn == 0 and first == 0 else parts_of(*there)
        for k, (start, size) in enumerate(copies):
            piece = span(array, first, second, start, size)
            send(piece, piece, ring_send, arrival(*there, k), near(axis, step))

    def cross(array, first, second, start, size):
        piece = span(array, first, second, start, size)
        send(piece, piece, core_sem.at[0], core_sem.at[1], partner)

    openings = list(starts())

    def first_sends():
        for chunk, axis, step, turn in openings:
            if turn == 0:
                pass_on(chunk, axis, step, turn)
        blocks(close_piece)
        for chunk, axis, step, turn in openings:
            if turn == 1:
                pass_on(chunk, axis, step, turn)

    def from_ahead(side, first, start, size):
        def work(at):
            for array in (0, 1):
                scaled(array, ahead.at[side, array], start, start_of(array, first, 0), size, at)

        blocks(work)

    sides = ((0, -1), (1, 1))
    more, left = AHEAD - part, 2 * part - AHEAD

    def take_early():
        for side, first in sides:
            await_bytes(ahead.at[side, :, pl.ds(0, part)], ahead_recv.at[2 * side])
            from_ahead(side, first, side * part, part)

    def take_late():
        for side, first in sides:
            await_bytes(ahead.at[side, :, pl.ds(0, more)], ahead_recv.at[2 * side + 1])
            from_ahead(side, first, left if side else part, more)

    @pl.when(core == 0)
    def _():
        first_sends()
        take_early()

    @pl.when(core == 1)
    def _():
        take_early()
        take_late()
        first_sends()

    gain_over_x()
    for array in (0, 1):
        for cut in range(CUTS):
            cross(array, 0, 0, cut * part, part)

    last = []
    for (array, first, second, cut), came_early in arrivals():
        if array == 1:
            continue
        if (first, second) == (2, 2):
            last.append(cut)
            continue
        if second == 0 and first in (1, -1) and not came_early:
            if first == -1:
                pl.when(core == 0)(take_late)
            await_bytes(big_g.at[pl.ds(0, 2 * left)], arrival(first, second, cut))
            if first == 1:
                gain_over_y()
        elif not came_early:
            await_bytes(big_g.at[pl.ds(0, 2 * part)], arrival(first, second, cut))
        for a in (0, 1):
            for axis, step, turn in onward(a, first, second, cut):
                pass_on((a, first, second, cut), axis, step, turn)
            cross(a, first, second, cut * part, part)
        if (first, second, cut) == (-1, 1, 1):
            gain_over_z()
    for k in (0, 1):
        for cut in last:
            start, size = parts_of(2, 2, cut)[k]
            await_bytes(big_g.at[pl.ds(0, 2 * size)], arrival(2, 2, cut, k))
            for a in (0, 1):
                cross(a, 2, 2, start, size)

    @pl.when(z > 0)
    def _():
        await_bytes(norm_whole, norm_recv.at[3])
        await_bytes(norm_z.at[0], norm_send.at[0])

    @pl.when(z == 0)
    def _():
        await_bytes(norm_x, norm_send.at[1])
        await_bytes(norm_y.at[pl.ds(0, 7)], norm_send.at[2])
        await_bytes(y_buf.at[pl.ds(0, 3)], norm_send.at[3])

    await_bytes(y_buf, small_send.at[0])
    await_bytes(z_buf.at[pl.ds(0, 7)], small_send.at[1])
    await_bytes(ahead.at[:, :, pl.ds(0, AHEAD)], ahead_send)
    passed = 2 * (SIDE * SIDE - 1) * rows - 4 * AHEAD
    await_bytes(big_g.at[pl.ds(0, passed)], ring_send)
    await_bytes(big_g, core_sem.at[0])
    await_bytes(big_u, core_sem.at[1])


def deliver(
    big_g, big_u, whole, scales,
    serving_g, serving_u, scale_g, scale_u, serve_norm, whole_g, whole_u, norm, sem,
):
    columns = big_g.shape[1]
    copies = []

    def put(src, dst):
        copies.append(pltpu.make_async_copy(src, dst, sem.at[len(copies)]))
        copies[-1].start()

    step = big_g.shape[0] // PARTS
    for src, dst in ((big_g, serving_g), (big_u, serving_u)):
        for k in range(PARTS):
            put(src.at[pl.ds(k * step, step)], dst.at[pl.ds(k * step, step)])
    put(whole.at[0], whole_g)
    put(whole.at[1], whole_u)
    put(scales.at[0, :, pl.ds(0, columns)], scale_g)
    put(scales.at[1, :, pl.ds(0, columns)], scale_u)
    norm[...] = scales[0, :, columns:].astype(jnp.bfloat16).reshape(-1)
    put(norm, serve_norm)
    for copy in copies:
        copy.wait()


def body(wg, mg, sg, wu, mu, su, norm_train, norm_step):
    rows, columns = wg.shape
    total = rows * lax.axis_size("shard")
    chunks = CUTS * (SIDE * SIDE - 1)
    f32, bf16 = jnp.float32, jnp.bfloat16
    hbm, vmem = pl.BlockSpec(memory_space=pltpu.HBM), pl.BlockSpec(memory_space=pltpu.VMEM)
    dma = pltpu.SemaphoreType.DMA
    gathered = pl.pallas_call(
        kernel,
        out_shape=(
            pltpu.VMEM((total, columns), bf16),
            pltpu.VMEM((total, columns), bf16),
            pltpu.VMEM((2, rows, columns), f32),
            pltpu.VMEM((2, 1, columns + SIDE * SIDE * LANES), f32),
        ),
        in_specs=[hbm] * 8,
        out_specs=(vmem,) * 4,
        scratch_shapes=[
            pltpu.VMEM((3, 2, rows, columns), f32),
            pltpu.VMEM((2, 1, columns), f32),
            pltpu.VMEM((7, 1, columns), f32),
            pltpu.VMEM((2 * SIDE, 1, columns), f32),
            pltpu.VMEM((2, 2, rows, columns), f32),
            pltpu.VMEM((2, 1, 16), f32),
            pltpu.VMEM((1, LANES), f32),
            pltpu.VMEM((SIDE, 1, LANES), f32),
            pltpu.VMEM((3, SIDE, 1, LANES), f32),
            pltpu.VMEM((2 * SIDE, SIDE, 1, LANES), f32),
            dma((5,)),
            dma((2,)),
            dma((2,)),
            dma((4,)),
            dma((4,)),
            dma,
            dma((4,)),
            dma,
            dma((chunks,)),
            dma((2,)),
        ],
        compiler_params=pltpu.CompilerParams(
            collective_id=0, has_side_effects=True, vmem_limit_bytes=47 * 1024 * 1024 - 300 * 1024
        ),
    )(wg, mg, sg, wu, mu, su, norm_train.reshape(1, -1), norm_step.reshape(1, -1))
    serving_g, serving_u, scale_g, scale_u, norm, whole_g, whole_u = pl.pallas_call(
        deliver,
        out_shape=(
            jax.ShapeDtypeStruct((total, columns), bf16),
            jax.ShapeDtypeStruct((total, columns), bf16),
            jax.ShapeDtypeStruct((1, columns), f32),
            jax.ShapeDtypeStruct((1, columns), f32),
            jax.ShapeDtypeStruct((total,), bf16),
            jax.ShapeDtypeStruct((rows, columns), f32),
            jax.ShapeDtypeStruct((rows, columns), f32),
        ),
        in_specs=[vmem] * 4,
        out_specs=(hbm,) * 7,
        scratch_shapes=[pltpu.VMEM((total,), bf16), dma((2 * PARTS + 5,))],
        compiler_params=pltpu.CompilerParams(vmem_limit_bytes=24 * 1024 * 1024),
    )(*gathered)
    return (
        serving_g,
        serving_u,
        scale_g.reshape(-1),
        scale_u.reshape(-1),
        norm,
        whole_g,
        whole_u,
    )


def solution(mesh):
    both = P("shard", "width")
    flat = P(("shard", "width"))
    wide = P(None, "width")
    return jax.shard_map(
        body,
        mesh=mesh,
        in_specs=(both,) * 6 + (flat, flat),
        out_specs=(wide, wide, P("width"), P("width"), P(), both, both),
        check_vma=False,
    )
```

```python
import heapq

import jax
import jax.numpy as jnp
from jax import lax
from jax.experimental import pallas as pl
from jax.experimental.pallas import tpu as pltpu
from jax.sharding import PartitionSpec as P

MESH = pl.DeviceIdType.MESH

learn_rate = 0.02
decay_rate = 0.1
tiny_value = 1e-08

SIDE = 4
CUTS = 2
LANES = 128
UNROLL = 4
PARTS = 2
AHEAD = 48
FIRST = 24
REST = 0.5


def axis_of(array, turn):
    return array if turn == 0 else 1 - array


def onward(array, first, second, cut):
    low = cut < CUTS // 2
    out = []
    if second == 0:
        if first == 0:
            out += [(0, 1), (0, -1)]
        elif first == -1 and low:
            out += [(0, 1)]
        elif first == 1 and not low:
            out += [(0, -1)]
        out += [(1, 1), (1, -1)]
    elif second == -1 and low:
        out += [(1, 1)]
    elif second == 1 and not low:
        out += [(1, -1)]
    return [(axis_of(array, turn), step, turn) for turn, step in out]


def moved(first, second, turn, step):
    def one(offset):
        return {0: -step, -step: 2}[offset]

    return (one(first), second) if turn == 0 else (first, one(second))


def early(array, step):
    return 0 if step == 1 else CUTS - 1


def rest(array, step, part):
    return (AHEAD, 2 * part - AHEAD) if step == 1 else (0, 2 * part - AHEAD)


def starts():
    for turn in (0, 1):
        for position in range(CUTS):
            for array in (0, 1):
                for axis, step, its_turn in onward(array, 0, 0, 0):
                    cut = position if step == 1 else CUTS - 1 - position
                    if its_turn == turn and not (turn == 0 and cut == early(array, step)):
                        yield (array, 0, 0, cut), axis, step, turn


def arrivals():
    free = {}
    queue = []
    order = []
    span, delay = 1.0, 0.7

    def send(chunk, axis, step, turn, now):
        array, first, second, cut = chunk
        own_rest = turn == 0 and first == 0
        done = max(free.get((axis, step), 0.0), now) + (REST if own_rest else span)
        free[axis, step] = done
        heapq.heappush(queue, (done + delay, (array, *moved(first, second, turn, step), cut)))

    for chunk, axis, step, turn in starts():
        send(chunk, axis, step, turn, 0.0)
    for array in (0, 1):
        for step in (1, -1):
            heapq.heappush(queue, (0.0, (array, -step, 0, early(array, step))))
    while queue:
        now, chunk = heapq.heappop(queue)
        order.append((chunk, now))
        for axis, step, turn in onward(*chunk):
            send(chunk, axis, step, turn, now)
    return order


def kernel(
    wg, mg, sg, wu, mu, su, norm_train, norm_step,
    big_g, big_u, whole, scales,
    loaded, local_max, y_buf, z_buf, ahead, norm_in, norm_row, norm_z, norm_x, norm_y,
    in_sem, small_send, small_recv, norm_send, norm_recv, ahead_send, ahead_recv, ring_send, ring_recv, core_sem,
):
    rows, columns = wg.shape
    part = rows // CUTS
    me, x = lax.axis_index("shard"), lax.axis_index("width")
    core = lax.rem(me, 2)
    y = lax.rem(lax.div(me, 2), SIDE)
    z = lax.div(me, 2 * SIDE)

    def device(dz=0, dy=0, flip=0):
        zz, yy = lax.rem(z + dz + SIDE, SIDE), lax.rem(y + dy + SIDE, SIDE)
        cc = 1 - core if flip else core
        return (zz * SIDE + yy) * 2 + cc

    def near(axis, step):
        return (device(dy=step) if axis == 0 else device(dz=step), x)

    partner = (device(flip=1), x)
    steps = [(k, flip) for k in (2, 1, 3) for flip in (0, 1)] + [(0, 1)]
    x_peers = [(me, lax.rem(x + k, SIDE)) for k in (1, 2, 3)]
    y_peers = [(device(dy=k, flip=f), x) for k, f in steps]
    z_peers = [(device(dz=k, flip=f), x) for k, f in steps]
    peers = y_peers + z_peers[:-1]

    half = columns // 2
    for a, refs in enumerate(((wg, mg, sg), (wu, mu, su))):
        for h in (0, 1):
            at = pl.ds(h * half, half)
            for k, src in enumerate(refs):
                pltpu.make_async_copy(src.at[:, at], loaded.at[k, a, :, at], in_sem.at[2 * a + h]).start()
    for k, src in enumerate((norm_train, norm_step)):
        pltpu.make_async_copy(src, norm_in.at[k], in_sem.at[4]).start()

    barrier = pltpu.get_barrier_semaphore()
    for peer in peers:
        pl.semaphore_signal(barrier, inc=1, device_id=peer, device_id_type=MESH)

    @pl.when(z == 0)
    def _():
        for peer in x_peers:
            pl.semaphore_signal(barrier, inc=1, device_id=peer, device_id_type=MESH)

    def await_bytes(ref, sem):
        pltpu.make_async_copy(ref, ref, sem).wait()

    for a in (0, 1):
        for h in (0, 1):
            await_bytes(loaded.at[:, a, :, pl.ds(h * half, half)], in_sem.at[2 * a + h])

            @pl.loop(0, half // LANES, unroll=UNROLL)
            def _(j):
                at = pl.ds(pl.multiple_of(h * half + j * LANES, LANES), LANES)
                weight, moment, square = (loaded[k, a, :, at] for k in range(3))
                root = square * lax.rsqrt(square) + tiny_value
                new = weight * (1.0 - learn_rate * decay_rate) - (learn_rate * moment) / root
                whole[a, :, at] = new
                local_max[a, :, at] = jnp.max(jnp.abs(new), axis=0, keepdims=True)

    await_bytes(norm_in, in_sem.at[4])
    gain = norm_in[0] + norm_in[1]
    for k in range(8):
        norm_row[:, 16 * k : 16 * (k + 1)] = gain
    lane = lax.broadcasted_iota(jnp.int32, (1, LANES), 1)
    mine = lax.div(lane, 16) == core * SIDE + x
    norm_z[z] = jnp.where(mine, norm_row[...], 0.0)

    pl.semaphore_wait(barrier, len(peers) + len(x_peers) * lax.div(SIDE - z, SIDE))

    def send(src, dst, send_sem, recv_sem, peer):
        pltpu.make_async_remote_copy(
            src_ref=src,
            dst_ref=dst,
            send_sem=send_sem,
            recv_sem=recv_sem,
            device_id=peer,
            device_id_type=MESH,
        ).start()

    def small(stage, src, dst, peer):
        send(src, dst, small_send.at[stage], small_recv.at[stage], peer)

    for k, flip in steps:
        a = 1 - core if flip else core
        small(0, local_max.at[a], y_buf.at[2 * ((SIDE - k) % SIDE) + flip - 1], (device(dy=k, flip=flip), x))

    def gain(stage, src, dst, peer):
        send(src, dst, norm_send.at[stage], norm_recv.at[stage], peer)

    norm_whole = scales.at[0, :, pl.ds(columns, SIDE * SIDE * LANES)]

    def gain_over_x():
        @pl.when(z == 0)
        def _():
            await_bytes(norm_z.at[pl.ds(0, 3)], norm_recv.at[0])
            for k, peer in enumerate(x_peers):
                gain(1, norm_z, norm_x.at[k], peer)

    def gain_over_y():
        @pl.when(z == 0)
        def _():
            await_bytes(norm_x, norm_recv.at[1])
            slot = SIDE * core + y
            norm_y[slot] = norm_z[...] + norm_x[0] + norm_x[1] + norm_x[2]
            for peer in y_peers:
                gain(2, norm_y.at[slot], norm_y.at[slot], peer)

    def gain_over_z():
        @pl.when(z == 0)
        def _():
            await_bytes(norm_y.at[pl.ds(0, 7)], norm_recv.at[2])
            for k in range(SIDE):
                for i in range(SIDE):
                    at = columns + (k * SIDE + i) * LANES
                    scales[0, :, at : at + LANES] = norm_y[i, k] + norm_y[SIDE + i, k]
            for k in (1, 2, 3):
                gain(3, norm_whole, norm_whole, (device(dz=k), x))

    @pl.when(z > 0)
    def _():
        gain(0, norm_z.at[z], norm_z.at[z], (device(dz=-z), x))

    def send_ahead(array, low, high, late):
        for step in (1, -1):
            side = int(step == -1)
            where = pl.ds(low if step == 1 else rows - high, high - low)
            send(
                whole.at[array, where],
                ahead.at[side, array, where],
                ahead_send,
                ahead_recv.at[2 * side + late],
                near(array, step),
            )

    send_ahead(1, 0, FIRST, 0)
    send_ahead(0, 0, part, 0)
    send_ahead(0, part, AHEAD, 1)
    await_bytes(y_buf, small_recv.at[0])
    best = local_max[core]
    for k in range(7):
        best = jnp.maximum(best, y_buf[k])
    here = SIDE * core + z
    z_buf[here] = best
    for k, flip in steps:
        small(1, z_buf.at[here], z_buf.at[here], (device(dz=k, flip=flip), x))
    send_ahead(1, FIRST, part, 0)
    send_ahead(1, part, AHEAD, 1)
    await_bytes(z_buf.at[pl.ds(0, 7)], small_recv.at[1])

    big = (big_g, big_u)
    own = pl.multiple_of(me * rows, rows)

    def scaled(array, src, start, base, size, at):
        factor = 1.0 / scales[array, :, at]
        there = pl.ds(pl.multiple_of(base + start, 8), size)
        big[array][there, at] = (src[pl.ds(start, size), at] * factor).astype(jnp.bfloat16)

    def blocks(work):
        @pl.loop(0, columns // LANES, unroll=UNROLL)
        def _(j):
            work(pl.ds(pl.multiple_of(j * LANES, LANES), LANES))

    def open_piece(at):
        for a in (0, 1):
            first = SIDE * a
            scales[a, :, at] = jnp.maximum(
                jnp.maximum(z_buf[first, :, at], z_buf[first + 1, :, at]),
                jnp.maximum(z_buf[first + 2, :, at], z_buf[first + 3, :, at]),
            )
            for step in (1, -1):
                start, size = rest(a, step, part)
                scaled(a, whole.at[a], start, own, size, at)

    def close_piece(at):
        for a in (0, 1):
            scaled(a, whole.at[a], 2 * part - AHEAD, own, 2 * AHEAD - 2 * part, at)

    blocks(open_piece)

    rounds = {}
    for (array, *chunk), now in arrivals():
        if array == 0:
            rounds.setdefault(round(now, 3), []).append(tuple(chunk))
    names = {}
    for number, (now, chunks) in enumerate(rounds.items()):
        names.update({chunk: number for chunk in chunks})

    def arrival(first, second, cut, piece=0):
        return ring_recv.at[names[first, second, cut] + piece]

    def start_of(array, first, second):
        dy, dz = (first, second) if array == 0 else (second, first)
        return device(dz=dz, dy=dy) * rows

    def span(array, first, second, start, size):
        at = start_of(array, first, second) + start
        return big[array].at[pl.ds(pl.multiple_of(at, 8), size)]

    def parts_of(first, second, cut):
        pieces = 2 if first == 2 and second == 2 else 1
        size = part // pieces
        return [(cut * part + k * size, size) for k in range(pieces)]

    def pass_on(chunk, axis, step, turn):
        array, first, second, cut = chunk
        there = (*moved(first, second, turn, step), cut)
        copies = [rest(array, step, part)] if turn == 0 and first == 0 else parts_of(*there)
        for k, (start, size) in enumerate(copies):
            piece = span(array, first, second, start, size)
            send(piece, piece, ring_send, arrival(*there, k), near(axis, step))

    def cross(array, first, second, start, size):
        piece = span(array, first, second, start, size)
        send(piece, piece, core_sem.at[0], core_sem.at[1], partner)

    openings = list(starts())

    def first_sends():
        for chunk, axis, step, turn in openings:
            if turn == 0:
                pass_on(chunk, axis, step, turn)
        blocks(close_piece)
        for chunk, axis, step, turn in openings:
            if turn == 1:
                pass_on(chunk, axis, step, turn)

    def from_ahead(side, first, start, size):
        def work(at):
            for array in (0, 1):
                scaled(array, ahead.at[side, array], start, start_of(array, first, 0), size, at)

        blocks(work)

    sides = ((0, -1), (1, 1))
    more, left = AHEAD - part, 2 * part - AHEAD

    def take_early():
        for side, first in sides:
            await_bytes(ahead.at[side, :, pl.ds(0, part)], ahead_recv.at[2 * side])
            from_ahead(side, first, side * part, part)

    def take_late():
        for side, first in sides:
            await_bytes(ahead.at[side, :, pl.ds(0, more)], ahead_recv.at[2 * side + 1])
            from_ahead(side, first, left if side else part, more)

    @pl.when(core == 0)
    def _():
        first_sends()
        take_early()

    @pl.when(core == 1)
    def _():
        take_early()
        take_late()
        first_sends()

    gain_over_x()

    for now, chunks in rounds.items():
        if chunks[0][:2] == (2, 2):
            continue
        first, second, cut = chunks[0]
        if now > 0.0:
            size = part
            if second == 0 and first in (1, -1):
                pl.when(core == 0)(take_late)
                size = left
            await_bytes(big_g.at[pl.ds(0, 2 * size * len(chunks))], arrival(first, second, cut))
            if size == left:
                gain_over_y()
        for first, second, cut in chunks:
            for a in (0, 1):
                for axis, step, turn in onward(a, first, second, cut):
                    pass_on((a, first, second, cut), axis, step, turn)
                cross(a, first, second, cut * part, part)
        if (0, -1, 0) in chunks:
            for array in (0, 1):
                for cut in range(CUTS):
                    cross(array, 0, 0, cut * part, part)
        if (-1, 1, 1) in chunks:
            gain_over_z()
    for k in (0, 1):
        size = parts_of(2, 2, 0)[k][1]
        await_bytes(big_g.at[pl.ds(0, 2 * size * CUTS)], arrival(2, 2, 0, k))
        for cut in range(CUTS):
            for a in (0, 1):
                cross(a, 2, 2, *parts_of(2, 2, cut)[k])

    @pl.when(z > 0)
    def _():
        await_bytes(norm_whole, norm_recv.at[3])
        await_bytes(norm_z.at[0], norm_send.at[0])

    @pl.when(z == 0)
    def _():
        await_bytes(norm_x, norm_send.at[1])
        await_bytes(norm_y.at[pl.ds(0, 7)], norm_send.at[2])
        await_bytes(y_buf.at[pl.ds(0, 3)], norm_send.at[3])

    await_bytes(y_buf, small_send.at[0])
    await_bytes(z_buf.at[pl.ds(0, 7)], small_send.at[1])
    await_bytes(ahead.at[:, :, pl.ds(0, AHEAD)], ahead_send)
    passed = 2 * (SIDE * SIDE - 1) * rows - 4 * AHEAD
    await_bytes(big_g.at[pl.ds(0, passed)], ring_send)
    await_bytes(big_g, core_sem.at[0])
    await_bytes(big_u, core_sem.at[1])


def deliver(
    big_g, big_u, whole, scales,
    serving_g, serving_u, scale_g, scale_u, serve_norm, whole_g, whole_u, norm, sem,
):
    columns = big_g.shape[1]
    copies = []

    def put(src, dst):
        copies.append(pltpu.make_async_copy(src, dst, sem.at[len(copies)]))
        copies[-1].start()

    step = big_g.shape[0] // PARTS
    for src, dst in ((big_g, serving_g), (big_u, serving_u)):
        for k in range(PARTS):
            put(src.at[pl.ds(k * step, step)], dst.at[pl.ds(k * step, step)])
    put(whole.at[0], whole_g)
    put(whole.at[1], whole_u)
    put(scales.at[0, :, pl.ds(0, columns)], scale_g)
    put(scales.at[1, :, pl.ds(0, columns)], scale_u)
    norm[...] = scales[0, :, columns:].astype(jnp.bfloat16).reshape(-1)
    put(norm, serve_norm)
    for copy in copies:
        copy.wait()


def body(wg, mg, sg, wu, mu, su, norm_train, norm_step):
    rows, columns = wg.shape
    total = rows * lax.axis_size("shard")
    rounds = len({round(now, 3) for _, now in arrivals()}) + 1
    f32, bf16 = jnp.float32, jnp.bfloat16
    hbm, vmem = pl.BlockSpec(memory_space=pltpu.HBM), pl.BlockSpec(memory_space=pltpu.VMEM)
    dma = pltpu.SemaphoreType.DMA
    gathered = pl.pallas_call(
        kernel,
        out_shape=(
            pltpu.VMEM((total, columns), bf16),
            pltpu.VMEM((total, columns), bf16),
            pltpu.VMEM((2, rows, columns), f32),
            pltpu.VMEM((2, 1, columns + SIDE * SIDE * LANES), f32),
        ),
        in_specs=[hbm] * 8,
        out_specs=(vmem,) * 4,
        scratch_shapes=[
            pltpu.VMEM((3, 2, rows, columns), f32),
            pltpu.VMEM((2, 1, columns), f32),
            pltpu.VMEM((7, 1, columns), f32),
            pltpu.VMEM((2 * SIDE, 1, columns), f32),
            pltpu.VMEM((2, 2, rows, columns), f32),
            pltpu.VMEM((2, 1, 16), f32),
            pltpu.VMEM((1, LANES), f32),
            pltpu.VMEM((SIDE, 1, LANES), f32),
            pltpu.VMEM((3, SIDE, 1, LANES), f32),
            pltpu.VMEM((2 * SIDE, SIDE, 1, LANES), f32),
            dma((5,)),
            dma((2,)),
            dma((2,)),
            dma((4,)),
            dma((4,)),
            dma,
            dma((4,)),
            dma,
            dma((rounds,)),
            dma((2,)),
        ],
        compiler_params=pltpu.CompilerParams(
            collective_id=0, has_side_effects=True, vmem_limit_bytes=47 * 1024 * 1024 - 300 * 1024
        ),
    )(wg, mg, sg, wu, mu, su, norm_train.reshape(1, -1), norm_step.reshape(1, -1))
    serving_g, serving_u, scale_g, scale_u, norm, whole_g, whole_u = pl.pallas_call(
        deliver,
        out_shape=(
            jax.ShapeDtypeStruct((total, columns), bf16),
            jax.ShapeDtypeStruct((total, columns), bf16),
            jax.ShapeDtypeStruct((1, columns), f32),
            jax.ShapeDtypeStruct((1, columns), f32),
            jax.ShapeDtypeStruct((total,), bf16),
            jax.ShapeDtypeStruct((rows, columns), f32),
            jax.ShapeDtypeStruct((rows, columns), f32),
        ),
        in_specs=[vmem] * 4,
        out_specs=(hbm,) * 7,
        scratch_shapes=[pltpu.VMEM((total,), bf16), dma((2 * PARTS + 5,))],
        compiler_params=pltpu.CompilerParams(vmem_limit_bytes=24 * 1024 * 1024),
    )(*gathered)
    return (
        serving_g,
        serving_u,
        scale_g.reshape(-1),
        scale_u.reshape(-1),
        norm,
        whole_g,
        whole_u,
    )


def solution(mesh):
    both = P("shard", "width")
    flat = P(("shard", "width"))
    wide = P(None, "width")
    return jax.shard_map(
        body,
        mesh=mesh,
        in_specs=(both,) * 6 + (flat, flat),
        out_specs=(wide, wide, P("width"), P("width"), P(), both, both),
        check_vma=False,
    )
```

```python
import heapq

import jax
import jax.numpy as jnp
from jax import lax
from jax.experimental import pallas as pl
from jax.experimental.pallas import tpu as pltpu
from jax.sharding import PartitionSpec as P

MESH = pl.DeviceIdType.MESH

learn_rate = 0.02
decay_rate = 0.1
tiny_value = 1e-08

SIDE = 4
CUTS = 2
LANES = 128
UNROLL = 8
PARTS = 2
AHEAD = 48
FIRST = 24
REST = 0.5


def axis_of(array, turn):
    return array if turn == 0 else 1 - array


def onward(array, first, second, cut):
    low = cut < CUTS // 2
    out = []
    if second == 0:
        if first == 0:
            out += [(0, 1), (0, -1)]
        elif first == -1 and low:
            out += [(0, 1)]
        elif first == 1 and not low:
            out += [(0, -1)]
        out += [(1, 1), (1, -1)]
    elif second == -1 and low:
        out += [(1, 1)]
    elif second == 1 and not low:
        out += [(1, -1)]
    return [(axis_of(array, turn), step, turn) for turn, step in out]


def moved(first, second, turn, step):
    def one(offset):
        return {0: -step, -step: 2}[offset]

    return (one(first), second) if turn == 0 else (first, one(second))


def early(array, step):
    return 0 if step == 1 else CUTS - 1


def rest(array, step, part):
    return (AHEAD, 2 * part - AHEAD) if step == 1 else (0, 2 * part - AHEAD)


def starts():
    for turn in (0, 1):
        for position in range(CUTS):
            for array in (0, 1):
                for axis, step, its_turn in onward(array, 0, 0, 0):
                    cut = position if step == 1 else CUTS - 1 - position
                    if its_turn == turn and not (turn == 0 and cut == early(array, step)):
                        yield (array, 0, 0, cut), axis, step, turn


def arrivals():
    free = {}
    queue = []
    order = []
    span, delay = 1.0, 0.7

    def send(chunk, axis, step, turn, now):
        array, first, second, cut = chunk
        own_rest = turn == 0 and first == 0
        done = max(free.get((axis, step), 0.0), now) + (REST if own_rest else span)
        free[axis, step] = done
        heapq.heappush(queue, (done + delay, (array, *moved(first, second, turn, step), cut)))

    for chunk, axis, step, turn in starts():
        send(chunk, axis, step, turn, 0.0)
    for array in (0, 1):
        for step in (1, -1):
            heapq.heappush(queue, (0.0, (array, -step, 0, early(array, step))))
    while queue:
        now, chunk = heapq.heappop(queue)
        order.append((chunk, now))
        for axis, step, turn in onward(*chunk):
            send(chunk, axis, step, turn, now)
    return order


def kernel(
    wg, mg, sg, wu, mu, su, norm_train, norm_step,
    big_g, big_u, whole, scales,
    loaded, local_max, y_buf, z_buf, ahead, norm_in, norm_row, norm_z, norm_x, norm_y,
    in_sem, small_send, small_recv, norm_send, norm_recv, ahead_send, ahead_recv, ring_send, ring_recv, core_sem,
):
    rows, columns = wg.shape
    part = rows // CUTS
    me, x = lax.axis_index("shard"), lax.axis_index("width")
    core = lax.rem(me, 2)
    y = lax.rem(lax.div(me, 2), SIDE)
    z = lax.div(me, 2 * SIDE)

    def device(dz=0, dy=0, flip=0):
        zz, yy = lax.rem(z + dz + SIDE, SIDE), lax.rem(y + dy + SIDE, SIDE)
        cc = 1 - core if flip else core
        return (zz * SIDE + yy) * 2 + cc

    def near(axis, step):
        return (device(dy=step) if axis == 0 else device(dz=step), x)

    partner = (device(flip=1), x)
    steps = [(k, flip) for flip in (1, 0) for k in (2, 1, 3)] + [(0, 1)]
    x_peers = [(me, lax.rem(x + k, SIDE)) for k in (1, 2, 3)]
    y_peers = [(device(dy=k, flip=f), x) for k, f in steps]
    z_peers = [(device(dz=k, flip=f), x) for k, f in steps]
    peers = y_peers + z_peers[:-1]

    half = columns // 2
    for a, refs in enumerate(((wg, mg, sg), (wu, mu, su))):
        for h in (0, 1):
            at = pl.ds(h * half, half)
            for k, src in enumerate(refs):
                pltpu.make_async_copy(src.at[:, at], loaded.at[k, a, :, at], in_sem.at[2 * a + h]).start()
    for k, src in enumerate((norm_train, norm_step)):
        pltpu.make_async_copy(src, norm_in.at[k], in_sem.at[4]).start()

    barrier = pltpu.get_barrier_semaphore()
    for peer in peers:
        pl.semaphore_signal(barrier, inc=1, device_id=peer, device_id_type=MESH)

    @pl.when(z == 0)
    def _():
        for peer in x_peers:
            pl.semaphore_signal(barrier, inc=1, device_id=peer, device_id_type=MESH)

    def await_bytes(ref, sem):
        pltpu.make_async_copy(ref, ref, sem).wait()

    for a in (0, 1):
        for h in (0, 1):
            await_bytes(loaded.at[:, a, :, pl.ds(h * half, half)], in_sem.at[2 * a + h])

            @pl.loop(0, half // LANES, unroll=UNROLL)
            def _(j):
                at = pl.ds(pl.multiple_of(h * half + j * LANES, LANES), LANES)
                weight, moment, square = (loaded[k, a, :, at] for k in range(3))
                root = square * lax.rsqrt(square) + tiny_value
                new = weight * (1.0 - learn_rate * decay_rate) - (learn_rate * moment) / root
                whole[a, :, at] = new
                local_max[a, :, at] = jnp.max(jnp.abs(new), axis=0, keepdims=True)

    await_bytes(norm_in, in_sem.at[4])
    gain = norm_in[0] + norm_in[1]
    for k in range(8):
        norm_row[:, 16 * k : 16 * (k + 1)] = gain
    lane = lax.broadcasted_iota(jnp.int32, (1, LANES), 1)
    mine = lax.div(lane, 16) == core * SIDE + x
    norm_z[z] = jnp.where(mine, norm_row[...], 0.0)

    pl.semaphore_wait(barrier, len(peers) + len(x_peers) * lax.div(SIDE - z, SIDE))

    def send(src, dst, send_sem, recv_sem, peer):
        pltpu.make_async_remote_copy(
            src_ref=src,
            dst_ref=dst,
            send_sem=send_sem,
            recv_sem=recv_sem,
            device_id=peer,
            device_id_type=MESH,
        ).start()

    def small(stage, src, dst, peer):
        send(src, dst, small_send.at[stage], small_recv.at[stage], peer)

    for k, flip in steps:
        a = 1 - core if flip else core
        small(0, local_max.at[a], y_buf.at[2 * ((SIDE - k) % SIDE) + flip - 1], (device(dy=k, flip=flip), x))

    def gain(stage, src, dst, peer):
        send(src, dst, norm_send.at[stage], norm_recv.at[stage], peer)

    norm_whole = scales.at[0, :, pl.ds(columns, SIDE * SIDE * LANES)]

    def gain_over_x():
        @pl.when(z == 0)
        def _():
            await_bytes(norm_z.at[pl.ds(0, 3)], norm_recv.at[0])
            for k, peer in enumerate(x_peers):
                gain(1, norm_z, norm_x.at[k], peer)

    def gain_over_y():
        @pl.when(z == 0)
        def _():
            await_bytes(norm_x, norm_recv.at[1])
            slot = SIDE * core + y
            norm_y[slot] = norm_z[...] + norm_x[0] + norm_x[1] + norm_x[2]
            for peer in y_peers:
                gain(2, norm_y.at[slot], norm_y.at[slot], peer)

    def gain_over_z():
        @pl.when(z == 0)
        def _():
            await_bytes(norm_y.at[pl.ds(0, 7)], norm_recv.at[2])
            for k in range(SIDE):
                for i in range(SIDE):
                    at = columns + (k * SIDE + i) * LANES
                    scales[0, :, at : at + LANES] = norm_y[i, k] + norm_y[SIDE + i, k]
            for k in (1, 2, 3):
                gain(3, norm_whole, norm_whole, (device(dz=k), x))

    @pl.when(z > 0)
    def _():
        gain(0, norm_z.at[z], norm_z.at[z], (device(dz=-z), x))

    def send_ahead(array, low, high, late):
        for step in (1, -1):
            side = int(step == -1)
            where = pl.ds(low if step == 1 else rows - high, high - low)
            send(
                whole.at[array, where],
                ahead.at[side, array, where],
                ahead_send,
                ahead_recv.at[2 * side + late],
                near(array, step),
            )

    send_ahead(1, 0, FIRST, 0)
    send_ahead(0, 0, part, 0)
    send_ahead(0, part, AHEAD, 1)
    await_bytes(y_buf, small_recv.at[0])
    best = local_max[core]
    for k in range(7):
        best = jnp.maximum(best, y_buf[k])
    here = SIDE * core + z
    z_buf[here] = best
    for k, flip in steps:
        small(1, z_buf.at[here], z_buf.at[here], (device(dz=k, flip=flip), x))
    send_ahead(1, FIRST, part, 0)
    send_ahead(1, part, AHEAD, 1)
    await_bytes(z_buf.at[pl.ds(0, 7)], small_recv.at[1])

    big = (big_g, big_u)
    own = pl.multiple_of(me * rows, rows)

    def scaled(array, src, start, base, size, at):
        factor = 1.0 / scales[array, :, at]
        there = pl.ds(pl.multiple_of(base + start, 8), size)
        big[array][there, at] = (src[pl.ds(start, size), at] * factor).astype(jnp.bfloat16)

    def blocks(work):
        @pl.loop(0, columns // LANES, unroll=UNROLL)
        def _(j):
            work(pl.ds(pl.multiple_of(j * LANES, LANES), LANES))

    def open_piece(at):
        for a in (0, 1):
            first = SIDE * a
            scales[a, :, at] = jnp.maximum(
                jnp.maximum(z_buf[first, :, at], z_buf[first + 1, :, at]),
                jnp.maximum(z_buf[first + 2, :, at], z_buf[first + 3, :, at]),
            )
            for step in (1, -1):
                start, size = rest(a, step, part)
                scaled(a, whole.at[a], start, own, size, at)

    def close_piece(at):
        for a in (0, 1):
            scaled(a, whole.at[a], 2 * part - AHEAD, own, 2 * AHEAD - 2 * part, at)

    blocks(open_piece)

    rounds = {}
    for (array, *chunk), now in arrivals():
        if array == 0:
            rounds.setdefault(round(now, 3), []).append(tuple(chunk))
    names = {}
    for number, (now, chunks) in enumerate(rounds.items()):
        names.update({chunk: number for chunk in chunks})

    def arrival(first, second, cut, piece=0):
        return ring_recv.at[names[first, second, cut] + piece]

    def start_of(array, first, second):
        dy, dz = (first, second) if array == 0 else (second, first)
        return device(dz=dz, dy=dy) * rows

    def span(array, first, second, start, size):
        at = start_of(array, first, second) + start
        return big[array].at[pl.ds(pl.multiple_of(at, 8), size)]

    def parts_of(first, second, cut):
        pieces = 2 if first == 2 and second == 2 else 1
        size = part // pieces
        return [(cut * part + k * size, size) for k in range(pieces)]

    def pass_on(chunk, axis, step, turn):
        array, first, second, cut = chunk
        there = (*moved(first, second, turn, step), cut)
        copies = [rest(array, step, part)] if turn == 0 and first == 0 else parts_of(*there)
        for k, (start, size) in enumerate(copies):
            piece = span(array, first, second, start, size)
            send(piece, piece, ring_send, arrival(*there, k), near(axis, step))

    def cross(array, first, second, start, size):
        piece = span(array, first, second, start, size)
        send(piece, piece, core_sem.at[0], core_sem.at[1], partner)

    openings = list(starts())

    def first_sends():
        for chunk, axis, step, turn in openings:
            if turn == 0:
                pass_on(chunk, axis, step, turn)
        blocks(close_piece)
        for chunk, axis, step, turn in openings:
            if turn == 1:
                pass_on(chunk, axis, step, turn)

    def from_ahead(side, first, start, size):
        def work(at):
            for array in (0, 1):
                scaled(array, ahead.at[side, array], start, start_of(array, first, 0), size, at)

        blocks(work)

    sides = ((0, -1), (1, 1))
    more, left = AHEAD - part, 2 * part - AHEAD

    def take_early():
        for side, first in sides:
            await_bytes(ahead.at[side, :, pl.ds(0, part)], ahead_recv.at[2 * side])
            from_ahead(side, first, side * part, part)

    def take_late():
        for side, first in sides:
            await_bytes(ahead.at[side, :, pl.ds(0, more)], ahead_recv.at[2 * side + 1])
            from_ahead(side, first, left if side else part, more)

    @pl.when(core == 0)
    def _():
        first_sends()
        take_early()

    @pl.when(core == 1)
    def _():
        take_early()
        take_late()
        first_sends()

    gain_over_x()

    for now, chunks in rounds.items():
        if chunks[0][:2] == (2, 2):
            continue
        first, second, cut = chunks[0]
        if now > 0.0:
            size = part
            if second == 0 and first in (1, -1):
                pl.when(core == 0)(take_late)
                size = left
            await_bytes(big_g.at[pl.ds(0, 2 * size * len(chunks))], arrival(first, second, cut))
            if size == left:
                gain_over_y()
        for first, second, cut in chunks:
            for a in (0, 1):
                for axis, step, turn in onward(a, first, second, cut):
                    pass_on((a, first, second, cut), axis, step, turn)
                cross(a, first, second, cut * part, part)
        if (0, -1, 0) in chunks:
            for array in (0, 1):
                for cut in range(CUTS):
                    cross(array, 0, 0, cut * part, part)
        if (-1, 1, 1) in chunks:
            gain_over_z()
    for k in (0, 1):
        size = parts_of(2, 2, 0)[k][1]
        await_bytes(big_g.at[pl.ds(0, 2 * size * CUTS)], arrival(2, 2, 0, k))
        for cut in range(CUTS):
            for a in (0, 1):
                cross(a, 2, 2, *parts_of(2, 2, cut)[k])

    @pl.when(z > 0)
    def _():
        await_bytes(norm_whole, norm_recv.at[3])
        await_bytes(norm_z.at[0], norm_send.at[0])

    @pl.when(z == 0)
    def _():
        await_bytes(norm_x, norm_send.at[1])
        await_bytes(norm_y.at[pl.ds(0, 7)], norm_send.at[2])
        await_bytes(y_buf.at[pl.ds(0, 3)], norm_send.at[3])

    await_bytes(y_buf, small_send.at[0])
    await_bytes(z_buf.at[pl.ds(0, 7)], small_send.at[1])
    await_bytes(ahead.at[:, :, pl.ds(0, AHEAD)], ahead_send)
    passed = 2 * (SIDE * SIDE - 1) * rows - 4 * AHEAD
    await_bytes(big_g.at[pl.ds(0, passed)], ring_send)
    await_bytes(big_g, core_sem.at[0])
    await_bytes(big_u, core_sem.at[1])


def deliver(
    big_g, big_u, whole, scales,
    serving_g, serving_u, scale_g, scale_u, serve_norm, whole_g, whole_u, norm, sem,
):
    columns = big_g.shape[1]
    copies = []

    def put(src, dst):
        copies.append(pltpu.make_async_copy(src, dst, sem.at[len(copies)]))
        copies[-1].start()

    step = big_g.shape[0] // PARTS
    for src, dst in ((big_g, serving_g), (big_u, serving_u)):
        for k in range(PARTS):
            put(src.at[pl.ds(k * step, step)], dst.at[pl.ds(k * step, step)])
    put(whole.at[0], whole_g)
    put(whole.at[1], whole_u)
    put(scales.at[0, :, pl.ds(0, columns)], scale_g)
    put(scales.at[1, :, pl.ds(0, columns)], scale_u)
    norm[...] = scales[0, :, columns:].astype(jnp.bfloat16).reshape(-1)
    put(norm, serve_norm)
    for copy in copies:
        copy.wait()


def body(wg, mg, sg, wu, mu, su, norm_train, norm_step):
    rows, columns = wg.shape
    total = rows * lax.axis_size("shard")
    rounds = len({round(now, 3) for _, now in arrivals()}) + 1
    f32, bf16 = jnp.float32, jnp.bfloat16
    hbm, vmem = pl.BlockSpec(memory_space=pltpu.HBM), pl.BlockSpec(memory_space=pltpu.VMEM)
    dma = pltpu.SemaphoreType.DMA
    gathered = pl.pallas_call(
        kernel,
        out_shape=(
            pltpu.VMEM((total, columns), bf16),
            pltpu.VMEM((total, columns), bf16),
            pltpu.VMEM((2, rows, columns), f32),
            pltpu.VMEM((2, 1, columns + SIDE * SIDE * LANES), f32),
        ),
        in_specs=[hbm] * 8,
        out_specs=(vmem,) * 4,
        scratch_shapes=[
            pltpu.VMEM((3, 2, rows, columns), f32),
            pltpu.VMEM((2, 1, columns), f32),
            pltpu.VMEM((7, 1, columns), f32),
            pltpu.VMEM((2 * SIDE, 1, columns), f32),
            pltpu.VMEM((2, 2, rows, columns), f32),
            pltpu.VMEM((2, 1, 16), f32),
            pltpu.VMEM((1, LANES), f32),
            pltpu.VMEM((SIDE, 1, LANES), f32),
            pltpu.VMEM((3, SIDE, 1, LANES), f32),
            pltpu.VMEM((2 * SIDE, SIDE, 1, LANES), f32),
            dma((5,)),
            dma((2,)),
            dma((2,)),
            dma((4,)),
            dma((4,)),
            dma,
            dma((4,)),
            dma,
            dma((rounds,)),
            dma((2,)),
        ],
        compiler_params=pltpu.CompilerParams(
            collective_id=0, has_side_effects=True, vmem_limit_bytes=47 * 1024 * 1024 - 300 * 1024
        ),
    )(wg, mg, sg, wu, mu, su, norm_train.reshape(1, -1), norm_step.reshape(1, -1))
    serving_g, serving_u, scale_g, scale_u, norm, whole_g, whole_u = pl.pallas_call(
        deliver,
        out_shape=(
            jax.ShapeDtypeStruct((total, columns), bf16),
            jax.ShapeDtypeStruct((total, columns), bf16),
            jax.ShapeDtypeStruct((1, columns), f32),
            jax.ShapeDtypeStruct((1, columns), f32),
            jax.ShapeDtypeStruct((total,), bf16),
            jax.ShapeDtypeStruct((rows, columns), f32),
            jax.ShapeDtypeStruct((rows, columns), f32),
        ),
        in_specs=[vmem] * 4,
        out_specs=(hbm,) * 7,
        scratch_shapes=[pltpu.VMEM((total,), bf16), dma((2 * PARTS + 5,))],
        compiler_params=pltpu.CompilerParams(vmem_limit_bytes=24 * 1024 * 1024),
    )(*gathered)
    return (
        serving_g,
        serving_u,
        scale_g.reshape(-1),
        scale_u.reshape(-1),
        norm,
        whole_g,
        whole_u,
    )


def solution(mesh):
    both = P("shard", "width")
    flat = P(("shard", "width"))
    wide = P(None, "width")
    return jax.shard_map(
        body,
        mesh=mesh,
        in_specs=(both,) * 6 + (flat, flat),
        out_specs=(wide, wide, P("width"), P("width"), P(), both, both),
        check_vma=False,
    )
```
